8 devices in a mesh: sp: 8 (over z, y, x, core).
Axes of the slice: x: 2, y: 2, z: 1, core: 2. Of those that a mesh axis runs over, the one named last changes fastest.
Arguments:
- x_in: bfloat16 [2048, 2048], P('sp')
- positions: int32 [2048], P('sp')
- d_out: bfloat16 [2048, 2048], P('sp')
- norm1_gain: bfloat16 [2048], P('sp')
- norm2_gain: bfloat16 [2048], P('sp')
- w_q: bfloat16 [2048, 32, 64], P('sp')
- w_k: bfloat16 [2048, 4, 64], P('sp')
- w_v: bfloat16 [2048, 4, 64], P('sp')
- w_o: bfloat16 [32, 64, 2048], P('sp')
- w_gate: bfloat16 [2048, 5632], P('sp')
- w_up: bfloat16 [2048, 5632], P('sp')
- w_down: bfloat16 [5632, 2048], P('sp')
Outputs:
- output 1: bfloat16 [2048, 2048], P('sp')
- output 2: bfloat16 [2048, 2048], P('sp')
- output 3: float32 [2048], P('sp')
- output 4: float32 [2048], P('sp')
- output 5: float32 [2048, 32, 64], P('sp')
- output 6: float32 [2048, 4, 64], P('sp')
- output 7: float32 [2048, 4, 64], P('sp')
- output 8: float32 [32, 64, 2048], P('sp')
- output 9: float32 [2048, 5632], P('sp')
- output 10: float32 [2048, 5632], P('sp')
- output 11: float32 [5632, 2048], P('sp')
All inputs are finite; a program needn't handle non-finite values.
Results may differ from the reference program's by a relative error of at most 0.0187894.
Values are sent between devices in bfloat16 or wider.
A program may use at most 1 GiB of HBM per device.

```python
import math
import jax
import jax.numpy as jnp
from jax import lax

MODEL_DIM = 2048
FFN_DIM = 5632
Q_HEADS = 32
KV_HEADS = 4
HEAD_DIM = 64
SEQ_LEN = 2048

ROPE_BASE = 10000.0
NORM_EPS = 1e-5
NEG_LARGE = -1e30
GROUP_SIZE = Q_HEADS // KV_HEADS
HALF_DIM = HEAD_DIM // 2


def setup_inputs(seed: int = 0) -> dict:
    key_list = jax.random.split(jax.random.key(seed), 12)
    qk_gain = math.log(SEQ_LEN / 4.0) ** 0.25

    def normal_draw(key_one, shape, scale_by):
        return (jax.random.normal(key_one, shape, jnp.float32) * scale_by).astype(jnp.bfloat16)

    def gain_draw(key_one):
        return (0.6 + 0.8 * jax.random.uniform(key_one, (MODEL_DIM,), jnp.float32)).astype(jnp.bfloat16)

    pos_gaps = jax.random.randint(key_list[1], (SEQ_LEN,), 1, 4, jnp.int32)
    positions = (jnp.cumsum(pos_gaps) - pos_gaps[0]).astype(jnp.int32)
    return {
        'x_in': normal_draw(key_list[0], (SEQ_LEN, MODEL_DIM), 1.0),
        'positions': positions,
        'd_out': normal_draw(key_list[2], (SEQ_LEN, MODEL_DIM), 1.0),
        'norm1_gain': gain_draw(key_list[3]),
        'norm2_gain': gain_draw(key_list[4]),
        'w_q': normal_draw(key_list[5], (MODEL_DIM, Q_HEADS, HEAD_DIM), qk_gain * MODEL_DIM ** -0.5),
        'w_k': normal_draw(key_list[6], (MODEL_DIM, KV_HEADS, HEAD_DIM), qk_gain * MODEL_DIM ** -0.5),
        'w_v': normal_draw(key_list[7], (MODEL_DIM, KV_HEADS, HEAD_DIM), MODEL_DIM ** -0.5),
        'w_o': normal_draw(key_list[8], (Q_HEADS, HEAD_DIM, MODEL_DIM), (Q_HEADS * HEAD_DIM) ** -0.5),
        'w_gate': normal_draw(key_list[9], (MODEL_DIM, FFN_DIM), MODEL_DIM ** -0.5),
        'w_up': normal_draw(key_list[10], (MODEL_DIM, FFN_DIM), MODEL_DIM ** -0.5),
        'w_down': normal_draw(key_list[11], (FFN_DIM, MODEL_DIM), FFN_DIM ** -0.5),
    }


def keep_bf16(values_in):
    return values_in.astype(jnp.bfloat16).astype(jnp.float32)


def rms_norm(hidden, gain_vec):
    inv_rms = lax.rsqrt(jnp.mean(hidden * hidden, axis=-1, keepdims=True) + NORM_EPS)
    return keep_bf16(hidden * inv_rms * gain_vec)


def apply_rope(values_in, cos_tab, sin_tab):
    first_half = values_in[..., :HALF_DIM]
    second_half = values_in[..., HALF_DIM:]
    return jnp.concatenate([first_half * cos_tab - second_half * sin_tab, second_half * cos_tab + first_half * sin_tab], axis=-1)


def head_attention(operands):
    q_head, k_head, v_head = operands
    scores = jnp.dot(q_head, k_head.T, preferred_element_type=jnp.float32) * HEAD_DIM ** -0.5
    causal = jnp.arange(SEQ_LEN)[:, None] >= jnp.arange(SEQ_LEN)[None, :]
    attn_probs = jax.nn.softmax(jnp.where(causal, scores, NEG_LARGE), axis=-1)
    return keep_bf16(jnp.dot(keep_bf16(attn_probs), v_head, preferred_element_type=jnp.float32))


def layer_forward(x_f32, cos_tab, sin_tab, gain_first, gain_second, wq_f32, wk_f32, wv_f32, wo_f32, gate_f32, up_f32, down_f32):
    normed = rms_norm(x_f32, gain_first)
    q_lin = keep_bf16(jnp.einsum('td,dhe->the', normed, wq_f32))
    k_lin = keep_bf16(jnp.einsum('td,dhe->the', normed, wk_f32))
    v_lin = keep_bf16(jnp.einsum('td,dhe->the', normed, wv_f32))
    queries = keep_bf16(apply_rope(q_lin, cos_tab, sin_tab))
    keys_rot = keep_bf16(apply_rope(k_lin, cos_tab, sin_tab))
    keys_full = jnp.repeat(keys_rot, GROUP_SIZE, axis=1)
    values_full = jnp.repeat(v_lin, GROUP_SIZE, axis=1)
    attn_heads = lax.map(jax.checkpoint(head_attention), (queries.transpose(1, 0, 2), keys_full.transpose(1, 0, 2), values_full.transpose(1, 0, 2)))
    attn_proj = jnp.einsum('hte,hed->td', attn_heads, wo_f32)
    hidden = keep_bf16(x_f32 + attn_proj)
    mlp_in = rms_norm(hidden, gain_second)
    gate_act = keep_bf16(jnp.dot(mlp_in, gate_f32, preferred_element_type=jnp.float32))
    up_act = keep_bf16(jnp.dot(mlp_in, up_f32, preferred_element_type=jnp.float32))
    glu_out = keep_bf16(jax.nn.silu(gate_act) * up_act)
    return keep_bf16(hidden + jnp.dot(glu_out, down_f32, preferred_element_type=jnp.float32))


def reference(x_in, positions, d_out, norm1_gain, norm2_gain, w_q, w_k, w_v, w_o, w_gate, w_up, w_down):
    inv_freq = 1.0 / (ROPE_BASE ** (jnp.arange(HALF_DIM, dtype=jnp.float32) * (2.0 / HEAD_DIM)))
    angles = positions.astype(jnp.float32)[:, None] * inv_freq[None, :]
    cos_tab = jnp.cos(angles)[:, None, :]
    sin_tab = jnp.sin(angles)[:, None, :]

    def forward_fn(x_f32, gain_first, gain_second, wq_f32, wk_f32, wv_f32, wo_f32, gate_f32, up_f32, down_f32):
        return layer_forward(x_f32, cos_tab, sin_tab, gain_first, gain_second, wq_f32, wk_f32, wv_f32, wo_f32, gate_f32, up_f32, down_f32)

    to_f32 = [tensor.astype(jnp.float32) for tensor in (x_in, norm1_gain, norm2_gain, w_q, w_k, w_v, w_o, w_gate, w_up, w_down)]
    y_f32, pullback = jax.vjp(forward_fn, to_f32[0], to_f32[1], to_f32[2], to_f32[3], to_f32[4], to_f32[5], to_f32[6], to_f32[7], to_f32[8], to_f32[9])
    grad_list = pullback(d_out.astype(jnp.float32))
    return (y_f32.astype(jnp.bfloat16), grad_list[0].astype(jnp.bfloat16), grad_list[1], grad_list[2], grad_list[3], grad_list[4], grad_list[5], grad_list[6], grad_list[7], grad_list[8], grad_list[9])
```

```python
import functools
import jax
import jax.numpy as jnp
from jax import lax
from jax.experimental import pallas as pl
from jax.experimental.pallas import tpu as pltpu
from jax.experimental.layout import Layout, with_layout_constraint
from jax.sharding import PartitionSpec as P

ROPE_BASE = 10000.0
NORM_EPS = 1e-5
NEG_LARGE = -1e30
BLOCK = 256
XOR_ORDER = (2, 4, 6, 3, 5, 7, 1)
B16 = jnp.bfloat16
F32 = jnp.float32


def inverse_rms(hidden):
    return lax.rsqrt(jnp.mean(hidden * hidden, axis=-1, keepdims=True) + NORM_EPS)


def rope_tables(positions, head_dim):
    half_dim = head_dim // 2
    inv_freq = 1.0 / (ROPE_BASE ** (jnp.arange(half_dim, dtype=F32) * (2.0 / head_dim)))
    angles = positions.astype(F32)[:, None] * inv_freq[None, :]
    return jnp.cos(angles)[:, None, :], jnp.sin(angles)[:, None, :]


def gated_unit(gate_pre, up_pre):
    return jax.nn.silu(gate_pre) * up_pre


def norm_backward(d_normed, hidden, inv_rms, gain):
    scaled = d_normed * gain
    row_dot = jnp.mean(scaled * hidden, axis=-1, keepdims=True)
    return inv_rms * scaled - hidden * (inv_rms * inv_rms * inv_rms * row_dot)


def stack_heads(block, heads, head_dim):
    return jnp.concatenate([block[:, h * head_dim:(h + 1) * head_dim] for h in range(heads)], axis=0)


def unstack_heads(rows, heads):
    size = rows.shape[0] // heads
    return jnp.concatenate([rows[h * size:(h + 1) * size] for h in range(heads)], axis=1)


def dot_f32(lhs, rhs, dims):
    return lax.dot_general(lhs, rhs, (dims, ((), ())), preferred_element_type=F32)


def causal_block(heads):
    shape = (heads * BLOCK, BLOCK)
    row = lax.broadcasted_iota(jnp.int32, shape, 0) % BLOCK
    col = lax.broadcasted_iota(jnp.int32, shape, 1)
    return row >= col


def attention_forward_kernel(heads, head_dim, scale, q_ref, k_ref, v_ref, o_ref, max_ref, inv_ref, score_ref, acc_ref):
    step = pl.program_id(0)
    queries = stack_heads(q_ref[...], heads, head_dim)
    last = pl.multiple_of(step * BLOCK, BLOCK)

    def scores_at(start):
        return dot_f32(queries, k_ref[pl.ds(start, BLOCK), :], ((1,), (1,))) * scale

    def fold(op, block):
        return op(block[:, :128], block[:, 128:])

    diag = jnp.where(causal_block(heads), scores_at(last), NEG_LARGE)
    score_ref[:, pl.ds(last, BLOCK)] = diag
    acc_ref[...] = fold(jnp.maximum, diag)

    @pl.loop(0, step)
    def _(j):
        start = pl.multiple_of(j * BLOCK, BLOCK)
        block = scores_at(start)
        score_ref[:, pl.ds(start, BLOCK)] = block
        acc_ref[...] = jnp.maximum(acc_ref[...], fold(jnp.maximum, block))

    row_max = jnp.max(acc_ref[...], axis=1, keepdims=True)
    max_ref[...] = row_max
    acc_ref[...] = jnp.zeros_like(acc_ref)

    @pl.loop(0, step + 1)
    def _(j):
        start = pl.multiple_of(j * BLOCK, BLOCK)
        block = jnp.exp(score_ref[:, pl.ds(start, BLOCK)] - row_max)
        score_ref[:, pl.ds(start, BLOCK)] = block
        acc_ref[...] += fold(jnp.add, block)

    inv_sum = 1.0 / jnp.sum(acc_ref[...], axis=1, keepdims=True)
    inv_ref[...] = inv_sum

    def weighted(j, total):
        start = pl.multiple_of(j * BLOCK, BLOCK)
        probs = (score_ref[:, pl.ds(start, BLOCK)] * inv_sum).astype(B16)
        return total + dot_f32(probs, v_ref[pl.ds(start, BLOCK), :], ((1,), (0,)))

    total = lax.fori_loop(0, step + 1, weighted, jnp.zeros((heads * BLOCK, head_dim), F32))
    o_ref[...] = unstack_heads(total.astype(B16), heads)


def attention_forward(q_rot, k_rot, v_lin, heads):
    seq_len, width = q_rot.shape
    head_dim = width // heads
    rows = heads * BLOCK
    steps = seq_len // BLOCK
    whole = pl.BlockSpec((seq_len, head_dim), lambda i: (0, 0))
    tokens = pl.BlockSpec((BLOCK, width), lambda i: (i, 0))
    stats = pl.BlockSpec((rows, 1), lambda i: (i, 0))
    stat_shape = jax.ShapeDtypeStruct((steps * rows, 1), F32)
    return pl.pallas_call(
        functools.partial(attention_forward_kernel, heads, head_dim, head_dim ** -0.5),
        grid=(steps,),
        out_shape=(jax.ShapeDtypeStruct((seq_len, width), B16), stat_shape, stat_shape),
        in_specs=[tokens, whole, whole],
        out_specs=(tokens, stats, stats),
        scratch_shapes=[pltpu.VMEM((rows, seq_len), F32), pltpu.VMEM((rows, 128), F32)],
        compiler_params=pltpu.CompilerParams(vmem_limit_bytes=48 * 1024 * 1024),
        cost_estimate=pl.CostEstimate(flops=20_000_000_000, bytes_accessed=4_000_000, transcendentals=8_000_000),
        name='attention_forward',
    )(q_rot, k_rot, v_lin)


def attention_backward_kernel(heads, head_dim, scale, q_ref, do_ref, k_ref, v_ref, max_ref, inv_ref, cos_ref, sin_ref, dq_ref, dk_ref, dv_ref, prob_ref, dp_ref, acc_ref, dk_acc, dv_acc):
    step = pl.program_id(0)
    queries = stack_heads(q_ref[...], heads, head_dim)
    d_out = stack_heads(do_ref[...], heads, head_dim)
    row_max = max_ref[...]
    inv_sum = inv_ref[...]
    last = pl.multiple_of(step * BLOCK, BLOCK)

    @pl.when(step == 0)
    def _():
        dk_acc[...] = jnp.zeros_like(dk_acc)
        dv_acc[...] = jnp.zeros_like(dv_acc)

    def scores_at(start):
        return dot_f32(queries, k_ref[pl.ds(start, BLOCK), :], ((1,), (1,))) * scale

    def first_pass(start, scores):
        probs = jnp.exp(scores - row_max) * inv_sum
        d_probs = dot_f32(d_out, v_ref[pl.ds(start, BLOCK), :], ((1,), (1,))).astype(B16)
        prob_ref[:, pl.ds(start, BLOCK)] = probs
        dp_ref[:, pl.ds(start, BLOCK)] = d_probs
        product = probs * d_probs.astype(F32)
        dv_acc[:, pl.ds(start, BLOCK)] += dot_f32(d_out, probs.astype(B16), ((0,), (0,)))
        return product[:, :128] + product[:, 128:]

    acc_ref[...] = first_pass(last, jnp.where(causal_block(heads), scores_at(last), NEG_LARGE))

    @pl.loop(0, step)
    def _(j):
        start = pl.multiple_of(j * BLOCK, BLOCK)
        acc_ref[...] += first_pass(start, scores_at(start))

    row_dot = jnp.sum(acc_ref[...], axis=1, keepdims=True)

    def second_pass(j, total):
        start = pl.multiple_of(j * BLOCK, BLOCK)
        at = pl.ds(start, BLOCK)
        d_scores = (prob_ref[:, at] * (dp_ref[:, at].astype(F32) - row_dot) * scale).astype(B16)
        dk_acc[:, at] += dot_f32(queries, d_scores, ((0,), (0,)))
        return total + dot_f32(d_scores, k_ref[at, :], ((1,), (0,)))

    total = lax.fori_loop(0, step + 1, second_pass, jnp.zeros((heads * BLOCK, head_dim), F32))
    d_rot = unstack_heads(total.astype(B16), heads).astype(F32)
    cos_lanes, sin_lanes = cos_ref[...], sin_ref[...]
    d_lin = [rotate_lanes(d_rot[:, i:i + 128], cos_lanes, -sin_lanes, head_dim) for i in range(0, heads * head_dim, 128)]
    dq_ref[...] = jnp.concatenate(d_lin, axis=1).T.astype(B16)

    @pl.when(step == pl.num_programs(0) - 1)
    def _():
        dk_ref[...] = dk_acc[...].astype(B16)
        dv_ref[...] = dv_acc[...].astype(B16)


def attention_backward(q_rot, d_attn, k_rot, v_lin, row_max, inv_sum, cos_lanes, sin_lanes, heads):
    seq_len, width = q_rot.shape
    head_dim = width // heads
    rows = heads * BLOCK
    steps = seq_len // BLOCK
    whole = pl.BlockSpec((seq_len, head_dim), lambda i: (0, 0))
    whole_t = pl.BlockSpec((head_dim, seq_len), lambda i: (0, 0))
    tokens = pl.BlockSpec((BLOCK, width), lambda i: (i, 0))
    stats = pl.BlockSpec((rows, 1), lambda i: (i, 0))
    grad_t = jax.ShapeDtypeStruct((head_dim, seq_len), B16)
    table = pl.BlockSpec((BLOCK, 128), lambda i: (i, 0))
    return pl.pallas_call(
        functools.partial(attention_backward_kernel, heads, head_dim, head_dim ** -0.5),
        grid=(steps,),
        out_shape=(jax.ShapeDtypeStruct((width, seq_len), B16), grad_t, grad_t),
        in_specs=[tokens, tokens, whole, whole, stats, stats, table, table],
        out_specs=(pl.BlockSpec((width, BLOCK), lambda i: (0, i)), whole_t, whole_t),
        scratch_shapes=[
            pltpu.VMEM((rows, seq_len), F32),
            pltpu.VMEM((rows, seq_len), B16),
            pltpu.VMEM((rows, 128), F32),
            pltpu.VMEM((head_dim, seq_len), F32),
            pltpu.VMEM((head_dim, seq_len), F32),
        ],
        compiler_params=pltpu.CompilerParams(vmem_limit_bytes=48 * 1024 * 1024),
        cost_estimate=pl.CostEstimate(flops=40_000_000_000, bytes_accessed=6_000_000, transcendentals=8_000_000),
        name='attention_backward',
    )(q_rot, d_attn, k_rot, v_lin, row_max, inv_sum, cos_lanes, sin_lanes)


def swap_halves(values, head_dim):
    half = head_dim // 2
    lanes = values.shape[1]
    lane = lax.broadcasted_iota(jnp.int32, values.shape, 1)
    return jnp.where(lane % head_dim < half, pltpu.roll(values, lanes - half, 1), pltpu.roll(values, half, 1))


def rotate_lanes(values, cos_lanes, sin_lanes, head_dim):
    return values * cos_lanes + swap_halves(values, head_dim) * sin_lanes


def qkv_kernel(head_dim, me_ref, x_ref, gain_ref, w_ref, cos_ref, sin_ref, q_ref, k_ref, v_ref, u_rows_ref, x_rows_ref):
    width = q_ref.shape[1]
    hidden = x_ref[...].astype(F32)
    inv_rms = inverse_rms(hidden)
    normed = (hidden * inv_rms * gain_ref[...]).astype(B16)
    own = pl.ds(pl.multiple_of(me_ref[0] * u_rows_ref.shape[1], 128), u_rows_ref.shape[1])
    scaled = x_ref[:, own].astype(F32) * inv_rms
    x_rows_ref[...] = scaled
    u_rows_ref[...] = (scaled * gain_ref[:, own]).astype(B16)
    lin = jnp.dot(normed, w_ref[...], preferred_element_type=F32).astype(B16)
    cos_lanes, sin_lanes = cos_ref[...], sin_ref[...]
    rotated = [rotate_lanes(lin[:, i:i + 128].astype(F32), cos_lanes, sin_lanes, head_dim).astype(B16) for i in range(0, width + 128, 128)]
    q_ref[...] = jnp.concatenate(rotated[:-1], axis=1)
    k_ref[...] = rotated[-1][:, :head_dim]
    v_ref[...] = lin[:, width + head_dim:]


def project_qkv(me, x_full, gain, w_qkv, cos_lanes, sin_lanes, head_dim):
    seq_len, model_dim = x_full.shape
    width = w_qkv.shape[1] - 2 * head_dim
    part = BLOCK

    def tile(cols):
        return pl.BlockSpec((BLOCK, cols), lambda i, me_ref: (i, 0))

    def whole(shape):
        return pl.BlockSpec(shape, lambda i, me_ref: (0, 0))

    return pl.pallas_call(
        functools.partial(qkv_kernel, head_dim),
        grid_spec=pltpu.PrefetchScalarGridSpec(
            num_scalar_prefetch=1,
            grid=(seq_len // BLOCK,),
            in_specs=[tile(model_dim), whole((1, model_dim)), whole(w_qkv.shape), tile(128), tile(128)],
            out_specs=(tile(width), tile(head_dim), tile(head_dim), tile(part), tile(part)),
        ),
        out_shape=(
            jax.ShapeDtypeStruct((seq_len, width), B16),
            jax.ShapeDtypeStruct((seq_len, head_dim), B16),
            jax.ShapeDtypeStruct((seq_len, head_dim), B16),
            jax.ShapeDtypeStruct((seq_len, part), B16),
            jax.ShapeDtypeStruct((seq_len, part), F32),
        ),
        compiler_params=pltpu.CompilerParams(vmem_limit_bytes=32 * 1024 * 1024),
        cost_estimate=pl.CostEstimate(flops=3_000_000_000, bytes_accessed=14_000_000, transcendentals=0),
        name='project_qkv',
    )(me.reshape(1), x_full, gain, w_qkv, cos_lanes, sin_lanes)


def hold_weights(me_ref, held_refs, block_refs):
    count = held_refs[0].shape[0]

    @pl.when(pl.program_id(0) == 0)
    def _():
        for i, held in enumerate(held_refs):
            for k, ref in zip((0,) + XOR_ORDER, block_refs[i * count:(i + 1) * count]):
                held[lax.bitwise_xor(me_ref[0], k)] = ref[0]

    return [held[...].reshape(count * held.shape[1], held.shape[2]) for held in held_refs]


def mlp_forward_kernel(me_ref, h_ref, gain_ref, down_ref, *refs):
    weight_refs, out_refs, held_refs = refs[:-8], refs[-8:-2], refs[-2:]
    m_ref, gate_ref, up_ref, glu_ref, y_left_ref, y_right_ref = out_refs
    w_gate, w_up = hold_weights(me_ref, held_refs, weight_refs)
    hidden = h_ref[...].astype(F32)
    mlp_in = (hidden * inverse_rms(hidden) * gain_ref[...]).astype(B16)
    m_ref[...] = mlp_in
    gate_ref[...] = gate = jnp.dot(mlp_in, w_gate, preferred_element_type=F32).astype(B16)
    up_ref[...] = up = jnp.dot(mlp_in, w_up, preferred_element_type=F32).astype(B16)
    glu_ref[...] = glu = gated_unit(gate.astype(F32), up.astype(F32)).astype(B16)
    half = y_left_ref.shape[1]
    y_left_ref[...] = jnp.dot(glu, down_ref[:, :half], preferred_element_type=F32)
    y_right_ref[...] = jnp.dot(glu, down_ref[:, half:], preferred_element_type=F32)


def mlp_backward_kernel(me_ref, gate_ref, up_ref, dy_ref, down_ref, *refs):
    weight_refs, (da_ref, db_ref, dm_ref), held_refs = refs[:-5], refs[-5:-2], refs[-2:]
    w_gate, w_up = hold_weights(me_ref, held_refs, weight_refs)
    gate, up = gate_ref[...].astype(F32), up_ref[...].astype(F32)
    d_glu = dot_f32(dy_ref[...], down_ref[...], ((1,), (1,))).astype(B16).astype(F32)
    sig = jax.nn.sigmoid(gate)
    silu = gate * sig
    da_ref[...] = d_gate = (d_glu * up * (sig + silu * (1.0 - sig))).astype(B16)
    db_ref[...] = d_up = (d_glu * silu).astype(B16)
    dm_ref[...] = dot_f32(d_gate, w_gate, ((1,), (1,))) + dot_f32(d_up, w_up, ((1,), (1,)))


def token_tile(cols):
    return pl.BlockSpec((BLOCK, cols), lambda i, me_ref: (i, 0))


def whole_block(shape):
    return pl.BlockSpec(shape, lambda i, me_ref: (0,) * len(shape))


def mlp_call(kernel, me, operands, operand_specs, weights, out_cols, out_types, flops):
    seq_len = operands[0].shape[0]
    count, rows, part = weights[0].shape
    own_spec = pl.BlockSpec((1, rows, part), lambda i, me_ref: (me_ref[0], 0, 0))
    came_spec = whole_block((1, rows, part))
    weight_specs = ([own_spec] + [came_spec] * (count - 1)) * 2
    return pl.pallas_call(
        kernel,
        grid_spec=pltpu.PrefetchScalarGridSpec(
            num_scalar_prefetch=1,
            grid=(seq_len // BLOCK,),
            in_specs=operand_specs + weight_specs,
            out_specs=tuple(token_tile(cols) for cols in out_cols),
            scratch_shapes=[pltpu.VMEM((count, rows, part), B16), pltpu.VMEM((count, rows, part), B16)],
        ),
        out_shape=tuple(jax.ShapeDtypeStruct((seq_len, cols), dtype) for cols, dtype in zip(out_cols, out_types)),
        compiler_params=pltpu.CompilerParams(vmem_limit_bytes=60 * 1024 * 1024),
        cost_estimate=pl.CostEstimate(flops=flops, bytes_accessed=40_000_000, transcendentals=2_000_000),
    )(me.reshape(1), *operands, *weights)


def ffn_grad_kernel(me_ref, m_ref, da_ref, db_ref, gate_ref, up_ref, da_t, db_t):
    @pl.when(pl.program_id(0) == 0)
    def _():
        da_t[...] = da_ref[...].T
        db_t[...] = db_ref[...].T

    gate_ref[0] = jnp.dot(da_t[...], m_ref[...], preferred_element_type=F32)
    up_ref[0] = jnp.dot(db_t[...], m_ref[...], preferred_element_type=F32)


def ffn_grads(me, mlp_in, d_gate_act, d_up_act, count):
    seq_len, model_dim = mlp_in.shape
    rows, part = model_dim // count, d_gate_act.shape[1]
    block = pl.BlockSpec((1, part, rows), lambda k, me_ref: (k, 0, 0))
    shape = jax.ShapeDtypeStruct((count, part, rows), F32)
    return pl.pallas_call(
        ffn_grad_kernel,
        grid_spec=pltpu.PrefetchScalarGridSpec(
            num_scalar_prefetch=1,
            grid=(count,),
            in_specs=[pl.BlockSpec((seq_len, rows), lambda k, me_ref: (0, lax.bitwise_xor(me_ref[0], k)))] + [whole_block((seq_len, part))] * 2,
            out_specs=(block, block),
            scratch_shapes=[pltpu.VMEM((part, seq_len), B16), pltpu.VMEM((part, seq_len), B16)],
        ),
        out_shape=(shape, shape),
        compiler_params=pltpu.CompilerParams(vmem_limit_bytes=40 * 1024 * 1024),
        cost_estimate=pl.CostEstimate(flops=12_000_000_000, bytes_accessed=26_000_000, transcendentals=0),
        name='ffn_grads',
    )(me.reshape(1), mlp_in, d_gate_act, d_up_act)


def join_kernel(me_ref, *refs):
    blocks, out_ref, held = refs[:-2], refs[-2], refs[-1]
    for k, ref in zip((0,) + XOR_ORDER, blocks):
        held[lax.bitwise_xor(me_ref[0], k)] = ref[0]
    count, width, rows = held.shape
    for pair in range(count // 2):
        out_ref[:, pair * 2 * width:(pair + 1) * 2 * width] = held[2 * pair:2 * pair + 2].reshape(2 * width, rows).T


def join_columns(me, blocks, came):
    count, width, rows = blocks.shape
    tile = 128
    spec = pl.BlockSpec((1, width, tile), lambda i, me_ref: (0, 0, i))
    return pl.pallas_call(
        join_kernel,
        grid_spec=pltpu.PrefetchScalarGridSpec(
            num_scalar_prefetch=1,
            grid=(rows // tile,),
            in_specs=[spec] * count,
            out_specs=pl.BlockSpec((tile, count * width), lambda i, me_ref: (i, 0)),
            scratch_shapes=[pltpu.VMEM((count, width, tile), blocks.dtype)],
        ),
        out_shape=jax.ShapeDtypeStruct((rows, count * width), blocks.dtype),
        compiler_params=pltpu.CompilerParams(vmem_limit_bytes=32 * 1024 * 1024),
        cost_estimate=pl.CostEstimate(flops=1_000_000, bytes_accessed=12_000_000, transcendentals=0),
        name='join_columns',
    )(me.reshape(1), blocks, *came)


def pair_heads_kernel(k_ref, v_ref, out_ref):
    width = k_ref.shape[1] // 4
    parts = [ref[:, h * width:(h + 1) * width] for h in range(4) for ref in (k_ref, v_ref)]
    out_ref[...] = jnp.concatenate(parts, axis=1)


def pair_heads(wk_rows, wv_rows):
    rows, cols = wk_rows.shape
    return pl.pallas_call(pair_heads_kernel, out_shape=jax.ShapeDtypeStruct((rows, 2 * cols), B16), name='pair_heads')(wk_rows, wv_rows)


def qkv_grad_kernel(width, head_dim, g_ref, u_ref, x_ref, wq_ref, wkv_ref, cos_ref, sin_ref, dwq_ref, dwkv_ref, du_ref, dg_ref, acc_ref, share_ref):
    step = pl.program_id(0)
    half = head_dim // 2

    @pl.when(step == 0)
    def _():
        acc_ref[...] = jnp.zeros_like(acc_ref)

    dq = g_ref[0, :width, :]
    dwq_ref[...] = jnp.dot(dq, u_ref[...], preferred_element_type=F32).T
    acc_ref[...] += jnp.dot(wq_ref[...], dq, preferred_element_type=F32)
    share = g_ref[0, width:width + 2 * head_dim, :].astype(F32)

    @pl.when(step % 2 == 0)
    def _():
        share_ref[...] = share

    @pl.when(step % 2 == 1)
    def _():
        summed = (share_ref[...] + share).astype(B16)
        first, second = summed[:half].astype(F32), summed[half:head_dim].astype(F32)
        cos_rows, sin_rows = cos_ref[...], sin_ref[...]
        dk = jnp.concatenate([first * cos_rows + second * sin_rows, second * cos_rows - first * sin_rows], axis=0).astype(B16)
        dkv = jnp.concatenate([dk, summed[head_dim:]], axis=0)
        dwkv_ref[...] = jnp.dot(dkv, u_ref[...], preferred_element_type=F32).T
        acc_ref[...] += jnp.dot(wkv_ref[...], dkv, preferred_element_type=F32)

    @pl.when(step == pl.num_programs(0) - 1)
    def _():
        d_normed = acc_ref[...].T.astype(B16)
        du_ref[...] = d_normed
        dg_ref[...] = jnp.sum(d_normed.astype(F32) * x_ref[...], axis=0, keepdims=True)


def qkv_grads(gathered, u_rows, x_rows, wq_rows, wkv_rows, cos_t, sin_t, head_dim):
    count, height, seq_len = gathered.shape
    rows = u_rows.shape[1]
    width = wq_rows.shape[1] // count

    def whole(shape):
        return pl.BlockSpec(shape, lambda e: (0, 0))

    return pl.pallas_call(
        functools.partial(qkv_grad_kernel, width, head_dim),
        grid=(count,),
        in_specs=[
            pl.BlockSpec((1, height, seq_len), lambda e: (e, 0, 0)),
            whole(u_rows.shape),
            whole(x_rows.shape),
            pl.BlockSpec((rows, width), lambda e: (0, e)),
            pl.BlockSpec((rows, 2 * head_dim), lambda e: (0, e // 2)),
            whole(cos_t.shape),
            whole(sin_t.shape),
        ],
        out_specs=(
            pl.BlockSpec((rows, width), lambda e: (0, e)),
            pl.BlockSpec((rows, 2 * head_dim), lambda e: (0, e // 2)),
            whole((seq_len, rows)),
            whole((1, rows)),
        ),
        out_shape=(
            jax.ShapeDtypeStruct(wq_rows.shape, F32),
            jax.ShapeDtypeStruct(wkv_rows.shape, F32),
            jax.ShapeDtypeStruct((seq_len, rows), B16),
            jax.ShapeDtypeStruct((1, rows), F32),
        ),
        scratch_shapes=[pltpu.VMEM((rows, seq_len), F32), pltpu.VMEM((2 * head_dim, seq_len), F32)],
        compiler_params=pltpu.CompilerParams(vmem_limit_bytes=40 * 1024 * 1024),
        cost_estimate=pl.CostEstimate(flops=5_000_000_000, bytes_accessed=24_000_000, transcendentals=0),
        name='qkv_grads',
    )(gathered, u_rows, x_rows, wq_rows, wkv_rows, cos_t, sin_t)


def solution(mesh):
    n_dev = mesh.shape['sp']
    gather_rows = functools.partial(lax.all_gather, axis_name='sp', axis=0, tiled=True)
    scatter_rows = functools.partial(lax.psum_scatter, axis_name='sp', scatter_dimension=0, tiled=True)
    swap_blocks = functools.partial(lax.all_to_all, axis_name='sp', split_axis=0, concat_axis=0, tiled=True)

    def send_blocks(others):
        others = lax.optimization_barrier(tuple(with_layout_constraint(other, Layout((0, 1, 2))) for other in others))
        came = []
        for k, other in zip(XOR_ORDER, others):
            came.append(with_layout_constraint(lax.ppermute(other, 'sp', [(i, i ^ k) for i in range(n_dev)]), Layout((0, 1, 2))))
        return came

    def pick_blocks(blocks):
        me = lax.axis_index('sp')
        return [lax.dynamic_index_in_dim(blocks, lax.bitwise_xor(me, k), axis=0, keepdims=True) for k in XOR_ORDER]

    def after(value, *others):
        return lax.optimization_barrier((value,) + others)[0]

    def to_tokens(columns):
        blocks = swap_blocks(columns.reshape(n_dev, -1, columns.shape[1]))
        return blocks.transpose(1, 0, 2).reshape(blocks.shape[1], -1)

    def layer_step(x_in, positions, d_out, norm1_gain, norm2_gain, w_q, w_k, w_v, w_o, w_gate, w_up, w_down):
        tokens, model_dim = x_in.shape
        rows = model_dim // n_dev
        seq_len = tokens * n_dev
        q_heads, head_dim = w_q.shape[1:]
        kv_heads = w_k.shape[1]
        heads = q_heads // n_dev
        width = heads * head_dim
        kv_repeat = n_dev // kv_heads
        ffn_part = w_down.shape[0]
        me = lax.axis_index('sp')
        own_rows = functools.partial(lax.dynamic_slice_in_dim, start_index=me * rows, slice_size=rows, axis=1)

        x_full = gather_rows(x_in)
        wq_rows = w_q.reshape(rows, q_heads * head_dim)
        wk_rows = w_k.reshape(rows, kv_heads * head_dim)
        wv_rows = w_v.reshape(rows, kv_heads * head_dim)
        wo_rows = w_o.reshape(width, model_dim)

        wq_blocks = wq_rows.reshape(rows, n_dev, width).transpose(1, 0, 2)
        wk_blocks = jnp.repeat(w_k.transpose(1, 0, 2), kv_repeat, axis=0)
        wv_blocks = jnp.repeat(w_v.transpose(1, 0, 2), kv_repeat, axis=0)
        qkv_blocks = jnp.concatenate([wq_blocks, wk_blocks, wv_blocks], axis=2)
        lane_width = qkv_blocks.shape[2]
        small = jnp.stack([norm1_gain, norm2_gain, (positions // 128).astype(B16), (positions % 128).astype(B16)])
        small = jnp.pad(small, ((0, 12), (0, lane_width - rows)))
        small = jnp.broadcast_to(small[None], (n_dev,) + small.shape)
        qkv_cols = swap_blocks(jnp.concatenate([qkv_blocks, small], axis=1))
        w_qkv = qkv_cols[:, :rows].reshape(model_dim, lane_width)
        gain1 = qkv_cols[:, rows, :rows].reshape(model_dim).astype(F32)
        gain2 = qkv_cols[:, rows + 1, :rows].reshape(model_dim).astype(F32)
        pos_all = (qkv_cols[:, rows + 2, :rows].astype(F32) * 128.0 + qkv_cols[:, rows + 3, :rows].astype(F32)).reshape(seq_len)

        wo_full = gather_rows(wo_rows)
        dy_full = gather_rows(d_out)
        gate_blocks = w_gate.reshape(rows, n_dev, ffn_part).transpose(1, 0, 2)
        up_blocks = w_up.reshape(rows, n_dev, ffn_part).transpose(1, 0, 2)
        gate_others, up_others = pick_blocks(gate_blocks), pick_blocks(up_blocks)
        gate_others, up_others, x_full = lax.optimization_barrier((gate_others, up_others, x_full))
        gate_came, up_came = send_blocks(gate_others), send_blocks(up_others)

        cos_tab, sin_tab = rope_tables(pos_all, head_dim)
        cos_tab, sin_tab = cos_tab[:, 0], sin_tab[:, 0]
        cos_lanes = jnp.tile(cos_tab, (1, 4))
        sin_lanes = jnp.tile(jnp.concatenate([-sin_tab, sin_tab], axis=1), (1, 2))
        q_rot, k_rot, v_lin, u_rows, x_rows = project_qkv(me, x_full, gain1[None], w_qkv, cos_lanes, sin_lanes, head_dim)
        attn_cols, row_max, inv_sum = attention_forward(q_rot, k_rot, v_lin, heads)
        attn_tok = to_tokens(attn_cols)
        hidden = (x_in.astype(F32) + jnp.dot(attn_tok, wo_full, preferred_element_type=F32)).astype(B16)
        h_full = gather_rows(hidden)
        wk_late, wv_late = lax.optimization_barrier((wk_rows, wv_rows, hidden))[:2]
        wkv_rows = pair_heads(wk_late, wv_late)
        weights = (gate_blocks, *gate_came, up_blocks, *up_came)
        half = model_dim // 2
        mlp_in, gate_act, up_act, glu_out, y_left, y_right = mlp_call(
            mlp_forward_kernel, me, (h_full, gain2[None], w_down),
            [token_tile(model_dim), whole_block((1, model_dim)), whole_block(w_down.shape)],
            weights, (model_dim, ffn_part, ffn_part, ffn_part, half, half), (B16, B16, B16, B16, F32, F32), 18_000_000_000)
        y_left = scatter_rows(y_left)
        d_gate_act, d_up_act, d_mlp_part = mlp_call(
            mlp_backward_kernel, me, (gate_act, up_act, dy_full, w_down),
            [token_tile(ffn_part), token_tile(ffn_part), token_tile(model_dim), whole_block(w_down.shape)],
            weights, (ffn_part, ffn_part, model_dim), (B16, B16, F32), 18_000_000_000)
        d_mlp_sum = scatter_rows(d_mlp_part)
        d_gate_blocks, d_up_blocks = ffn_grads(me, mlp_in, d_gate_act, d_up_act, n_dev)
        d_gate_came = send_blocks([d_gate_blocks[k:k + 1] for k in XOR_ORDER])
        d_down = jnp.einsum('tf,td->fd', glu_out, dy_full, preferred_element_type=F32)
        d_mlp_sum, y_right, d_down, d_up_blocks = lax.optimization_barrier((d_mlp_sum, y_right, d_down, d_up_blocks))
        d_mlp_in = d_mlp_sum.astype(B16).astype(F32)
        hidden_f = hidden.astype(F32)
        inv2 = inverse_rms(hidden_f)
        d_hidden = (d_out.astype(F32) + norm_backward(d_mlp_in, hidden_f, inv2, gain2)).astype(B16)
        d_g2_part = jnp.sum(d_mlp_in * hidden_f * inv2, axis=0)
        dh_full = gather_rows(d_hidden)
        d_gate = join_columns(me, d_gate_blocks, d_gate_came)
        d_up_blocks = after(d_up_blocks, dh_full)
        d_up = join_columns(me, d_up_blocks, send_blocks([d_up_blocks[k:k + 1] for k in XOR_ORDER]))

        d_attn = jnp.einsum('td,cd->tc', dh_full, wo_rows, preferred_element_type=F32).astype(B16)
        dq_t, dk_t, dv_t = attention_backward(q_rot, d_attn, k_rot, v_lin, row_max, inv_sum, cos_lanes, sin_lanes, heads)
        d_wo = jnp.einsum('tc,td->cd', attn_cols, dh_full, preferred_element_type=F32)
        piece_hi = lax.reduce_precision(d_g2_part, 8, 7)
        piece_mid = lax.reduce_precision(d_g2_part - piece_hi, 8, 7)
        piece_lo = lax.reduce_precision(d_g2_part - piece_hi - piece_mid, 8, 7)
        pieces = jnp.pad(jnp.stack([piece_hi, piece_mid, piece_lo]).astype(B16), ((0, 13), (0, 0)))
        dqkv_t = gather_rows(jnp.concatenate([dq_t, dk_t, dv_t, pieces], axis=0)).reshape(n_dev, width + 2 * head_dim + 16, seq_len)
        d_g2 = jnp.sum(own_rows(dqkv_t[:, width + 2 * head_dim:width + 2 * head_dim + 3].reshape(-1, seq_len)).astype(F32), axis=0)
        dqkv_t, y_right, d_wo, d_gate, d_up = lax.optimization_barrier((dqkv_t, y_right, d_wo, d_gate, d_up))
        y_right = scatter_rows(y_right)
        y_out = (hidden_f + jnp.concatenate([y_left, y_right], axis=1)).astype(B16)

        d_wq, d_wkv, d_norm_cols, d_g1 = qkv_grads(dqkv_t, u_rows, x_rows, wq_rows, wkv_rows, cos_tab.T, sin_tab.T, head_dim)
        d_wkv = d_wkv.reshape(rows, kv_heads, 2, head_dim)
        d_wk, d_wv = d_wkv[:, :, 0], d_wkv[:, :, 1]
        d_g1 = d_g1[0]
        d_normed = to_tokens(d_norm_cols).astype(F32)
        x_f32 = x_in.astype(F32)
        d_x = (d_hidden.astype(F32) + norm_backward(d_normed, x_f32, inverse_rms(x_f32), gain1)).astype(B16)
        return (y_out, d_x, d_g1, d_g2, d_wq.reshape(w_q.shape), d_wk.reshape(w_k.shape), d_wv.reshape(w_v.shape), d_wo.reshape(w_o.shape), d_gate, d_up, d_down)

    all_rows = P('sp')
    return jax.shard_map(layer_step, mesh=mesh, in_specs=(all_rows,) * 12, out_specs=(all_rows,) * 11, check_vma=False)
```

```python
import functools
import jax
import jax.numpy as jnp
from jax import lax
from jax.experimental import pallas as pl
from jax.experimental.pallas import tpu as pltpu
from jax.experimental.layout import Layout, with_layout_constraint
from jax.sharding import PartitionSpec as P

ROPE_BASE = 10000.0
NORM_EPS = 1e-5
NEG_LARGE = -1e30
BLOCK = 256
MLP_BLOCK = 512
MIB = 1024 * 1024
EARLY = 3
NOW = 3
FIRST = 2
XOR_ORDER = (2, 4, 6, 3, 5, 7, 1)
B16 = jnp.bfloat16
F32 = jnp.float32


def inverse_rms(hidden):
    return lax.rsqrt(jnp.mean(hidden * hidden, axis=-1, keepdims=True) + NORM_EPS)


def rope_tables(positions, head_dim):
    half_dim = head_dim // 2
    inv_freq = 1.0 / (ROPE_BASE ** (jnp.arange(half_dim, dtype=F32) * (2.0 / head_dim)))
    angles = positions.astype(F32)[:, None] * inv_freq[None, :]
    return jnp.cos(angles)[:, None, :], jnp.sin(angles)[:, None, :]


def cost(mega_flops):
    return pl.CostEstimate(flops=mega_flops * 1_000_000, bytes_accessed=20_000_000, transcendentals=0)


def gated_unit(gate_pre, up_pre):
    return jax.nn.silu(gate_pre) * up_pre


def norm_backward(d_normed, hidden, inv_rms, gain):
    scaled = d_normed * gain
    row_dot = jnp.mean(scaled * hidden, axis=-1, keepdims=True)
    return inv_rms * scaled - hidden * (inv_rms * inv_rms * inv_rms * row_dot)


def stack_heads(block, heads, head_dim):
    return jnp.concatenate([block[:, h * head_dim:(h + 1) * head_dim] for h in range(heads)], axis=0)


def unstack_heads(rows, heads):
    size = rows.shape[0] // heads
    return jnp.concatenate([rows[h * size:(h + 1) * size] for h in range(heads)], axis=1)


def dot_f32(lhs, rhs, dims):
    return lax.dot_general(lhs, rhs, (dims, ((), ())), preferred_element_type=F32)


def causal_block(heads):
    shape = (heads * BLOCK, BLOCK)
    row = lax.broadcasted_iota(jnp.int32, shape, 0) % BLOCK
    col = lax.broadcasted_iota(jnp.int32, shape, 1)
    return row >= col


def attention_forward_kernel(heads, head_dim, scale, q_ref, k_ref, v_ref, o_ref, max_ref, inv_ref, score_ref, acc_ref):
    step = pl.program_id(0)
    queries = stack_heads(q_ref[:], heads, head_dim)
    last = pl.multiple_of(step * BLOCK, BLOCK)

    def scores_at(start):
        return dot_f32(queries, k_ref[pl.ds(start, BLOCK), :], ((1,), (1,))) * scale

    def fold(op, block):
        return op(block[:, :128], block[:, 128:])

    diag = jnp.where(causal_block(heads), scores_at(last), NEG_LARGE)
    score_ref[:, pl.ds(last, BLOCK)] = diag
    acc_ref[:] = fold(jnp.maximum, diag)

    @pl.loop(0, step)
    def _(j):
        start = pl.multiple_of(j * BLOCK, BLOCK)
        block = scores_at(start)
        score_ref[:, pl.ds(start, BLOCK)] = block
        acc_ref[:] = jnp.maximum(acc_ref[:], fold(jnp.maximum, block))

    row_max = jnp.max(acc_ref[:], axis=1, keepdims=True)
    max_ref[:] = row_max
    acc_ref[:] = jnp.zeros_like(acc_ref)

    @pl.loop(0, step + 1)
    def _(j):
        start = pl.multiple_of(j * BLOCK, BLOCK)
        block = jnp.exp(score_ref[:, pl.ds(start, BLOCK)] - row_max)
        score_ref[:, pl.ds(start, BLOCK)] = block
        acc_ref[:] += fold(jnp.add, block)

    inv_sum = 1.0 / jnp.sum(acc_ref[:], axis=1, keepdims=True)
    inv_ref[:] = inv_sum

    def weighted(j, total):
        start = pl.multiple_of(j * BLOCK, BLOCK)
        probs = (score_ref[:, pl.ds(start, BLOCK)] * inv_sum).astype(B16)
        return total + dot_f32(probs, v_ref[pl.ds(start, BLOCK), :], ((1,), (0,)))

    total = lax.fori_loop(0, step + 1, weighted, jnp.zeros((heads * BLOCK, head_dim), F32))
    o_ref[:] = unstack_heads(total.astype(B16), heads)


def attention_forward(q_rot, k_rot, v_lin, heads):
    seq_len, width = q_rot.shape
    head_dim = width // heads
    rows = heads * BLOCK
    steps = seq_len // BLOCK
    whole = whole_block((seq_len, head_dim))
    tokens = pl.BlockSpec((BLOCK, width), lambda i: (i, 0))
    stats = pl.BlockSpec((rows, 1), lambda i: (i, 0))
    stat_shape = jax.ShapeDtypeStruct((steps * rows, 1), F32)
    return pl.pallas_call(
        functools.partial(attention_forward_kernel, heads, head_dim, head_dim ** -0.5),
        grid=(steps,),
        out_shape=(jax.ShapeDtypeStruct((seq_len, width), B16), stat_shape, stat_shape),
        in_specs=[tokens, whole, whole],
        out_specs=(tokens, stats, stats),
        scratch_shapes=[pltpu.VMEM((rows, seq_len), F32), pltpu.VMEM((rows, 128), F32)],
        compiler_params=pltpu.CompilerParams(vmem_limit_bytes=48 * MIB),
        cost_estimate=cost(20000),
        name='attention_forward',
    )(q_rot, k_rot, v_lin)


def attention_backward_kernel(heads, head_dim, scale, q_ref, do_ref, k_ref, v_ref, max_ref, inv_ref, cos_ref, sin_ref, dq_ref, dk_ref, dv_ref, prob_ref, dp_ref, acc_ref, dk_acc, dv_acc):
    step = pl.program_id(0)
    queries = stack_heads(q_ref[:], heads, head_dim)
    d_out = stack_heads(do_ref[:], heads, head_dim)
    row_max = max_ref[:]
    inv_sum = inv_ref[:]
    last = pl.multiple_of(step * BLOCK, BLOCK)

    @pl.when(step == 0)
    def _():
        dk_acc[:] = jnp.zeros_like(dk_acc)
        dv_acc[:] = jnp.zeros_like(dv_acc)

    def scores_at(start):
        return dot_f32(queries, k_ref[pl.ds(start, BLOCK), :], ((1,), (1,))) * scale

    def first_pass(start, scores):
        probs = jnp.exp(scores - row_max) * inv_sum
        d_probs = dot_f32(d_out, v_ref[pl.ds(start, BLOCK), :], ((1,), (1,))).astype(B16)
        prob_ref[:, pl.ds(start, BLOCK)] = probs
        dp_ref[:, pl.ds(start, BLOCK)] = d_probs
        product = probs * d_probs.astype(F32)
        dv_acc[:, pl.ds(start, BLOCK)] += dot_f32(d_out, probs.astype(B16), ((0,), (0,)))
        return product[:, :128] + product[:, 128:]

    acc_ref[:] = first_pass(last, jnp.where(causal_block(heads), scores_at(last), NEG_LARGE))

    @pl.loop(0, step)
    def _(j):
        start = pl.multiple_of(j * BLOCK, BLOCK)
        acc_ref[:] += first_pass(start, scores_at(start))

    row_dot = jnp.sum(acc_ref[:], axis=1, keepdims=True)

    def second_pass(j, total):
        start = pl.multiple_of(j * BLOCK, BLOCK)
        at = pl.ds(start, BLOCK)
        d_scores = (prob_ref[:, at] * (dp_ref[:, at].astype(F32) - row_dot) * scale).astype(B16)
        dk_acc[:, at] += dot_f32(queries, d_scores, ((0,), (0,)))
        return total + dot_f32(d_scores, k_ref[at, :], ((1,), (0,)))

    total = lax.fori_loop(0, step + 1, second_pass, jnp.zeros((heads * BLOCK, head_dim), F32))
    d_rot = unstack_heads(total.astype(B16), heads).astype(F32)
    cos_lanes, sin_lanes = cos_ref[:], sin_ref[:]
    d_lin = [rotate_lanes(d_rot[:, i:i + 128], cos_lanes, -sin_lanes, head_dim) for i in range(0, heads * head_dim, 128)]
    dq_ref[:] = jnp.concatenate(d_lin, axis=1).T.astype(B16)

    @pl.when(step == pl.num_programs(0) - 1)
    def _():
        dk_ref[:] = dk_acc[:].astype(B16)
        dv_ref[:] = dv_acc[:].astype(B16)


def attention_backward(q_rot, d_attn, k_rot, v_lin, row_max, inv_sum, cos_lanes, sin_lanes, heads):
    seq_len, width = q_rot.shape
    head_dim = width // heads
    rows = heads * BLOCK
    steps = seq_len // BLOCK
    whole = whole_block((seq_len, head_dim))
    whole_t = whole_block((head_dim, seq_len))
    tokens = pl.BlockSpec((BLOCK, width), lambda i: (i, 0))
    stats = pl.BlockSpec((rows, 1), lambda i: (i, 0))
    grad_t = jax.ShapeDtypeStruct((head_dim, seq_len), B16)
    table = pl.BlockSpec((BLOCK, 128), lambda i: (i, 0))
    return pl.pallas_call(
        functools.partial(attention_backward_kernel, heads, head_dim, head_dim ** -0.5),
        grid=(steps,),
        out_shape=(jax.ShapeDtypeStruct((width, seq_len), B16), grad_t, grad_t),
        in_specs=[tokens, tokens, whole, whole, stats, stats, table, table],
        out_specs=(pl.BlockSpec((width, BLOCK), lambda i: (0, i)), whole_t, whole_t),
        scratch_shapes=[
            pltpu.VMEM((rows, seq_len), F32),
            pltpu.VMEM((rows, seq_len), B16),
            pltpu.VMEM((rows, 128), F32),
            pltpu.VMEM((head_dim, seq_len), F32),
            pltpu.VMEM((head_dim, seq_len), F32),
        ],
        compiler_params=pltpu.CompilerParams(vmem_limit_bytes=48 * MIB),
        cost_estimate=cost(40000),
        name='attention_backward',
    )(q_rot, d_attn, k_rot, v_lin, row_max, inv_sum, cos_lanes, sin_lanes)


def peer_of(me, mask):
    result = 0
    for bit in (1, 2, 4):
        mine = lax.rem(me // bit, 2)
        result = result + bit * ((1 - mine) if mask & bit else mine)
    return result


def gather_kernel(split, src_ref, out_ref, send_sem, recv_sem, local_sem):
    me = lax.axis_index('sp')
    rows = src_ref.shape[0]
    across, along, other, diagonal = (peer_of(me, mask) for mask in (2, 4, 1, 6))
    barrier = pltpu.get_barrier_semaphore()
    for device in (across, along, other):
        pl.semaphore_signal(barrier, inc=1, device_id=(device,), device_id_type=pl.DeviceIdType.MESH)
    pl.semaphore_wait(barrier, 3)

    upper, lower = (0, split), (split, rows - split)

    def place(owner, part):
        return out_ref.at[pl.ds(pl.multiple_of(owner * rows + part[0], 16), part[1]), :]

    def own(part):
        return src_ref.at[pl.ds(part[0], part[1]), :]

    plan = [
        (own(upper), place(me, upper), along),
        (own(lower), place(me, lower), across),
        (own(lower), place(me, lower), along),
        (own(upper), place(me, upper), across),
        (own((0, rows)), place(me, (0, rows)), other),
        (place(along, upper), place(along, upper), across),
        (place(across, lower), place(across, lower), along),
        (place(along, upper), place(along, upper), other),
        (place(across, lower), place(across, lower), other),
        (place(along, lower), place(along, lower), other),
        (place(across, upper), place(across, upper), other),
        (place(diagonal, upper), place(diagonal, upper), other),
        (place(diagonal, lower), place(diagonal, lower), other),
    ]
    copies = [
        pltpu.make_async_remote_copy(src_ref=src, dst_ref=dst, send_sem=send_sem.at[i], recv_sem=recv_sem.at[i], device_id=(device,), device_id_type=pl.DeviceIdType.MESH)
        for i, (src, dst, device) in enumerate(plan)
    ]
    for i in range(5):
        copies[i].start()
    mine = pltpu.make_async_copy(src_ref, place(me, (0, rows)), local_sem)
    mine.start()
    for came, go in ((0, (5, 7)), (1, (6, 8)), (2, (9,)), (3, (10,)), (5, (11,)), (6, (12,))):
        copies[came].wait_recv()
        for i in go:
            copies[i].start()
    for i in (4, 7, 8, 9, 10, 11, 12):
        copies[i].wait_recv()
    for copy in copies:
        copy.wait_send()
    mine.wait()


def gather_blocks(block, collective_id):
    rows, cols = block.shape
    split = (rows // 2 + 15) // 16 * 16
    return pl.pallas_call(
        functools.partial(gather_kernel, split),
        out_shape=jax.ShapeDtypeStruct((8 * rows, cols), block.dtype),
        in_specs=[pl.BlockSpec(memory_space=pltpu.VMEM)],
        out_specs=pl.BlockSpec(memory_space=pl.ANY),
        scratch_shapes=[pltpu.SemaphoreType.DMA((13,)), pltpu.SemaphoreType.DMA((13,)), pltpu.SemaphoreType.DMA],
        compiler_params=pltpu.CompilerParams(collective_id=collective_id, has_side_effects=True),
        cost_estimate=cost(30000),
        name='gather_blocks',
    )(block)


def reduce_kernel(part_ref, out_ref, mine, came, first_a, first_b, last_a, last_b, send_sem, recv_sem, local_sem):
    me = lax.axis_index('sp')
    masks = (0, 2, 4, 6)
    across, along, other = (peer_of(me, mask) for mask in (2, 4, 1))
    barrier = pltpu.get_barrier_semaphore()
    for device in (across, along, other):
        pl.semaphore_signal(barrier, inc=1, device_id=(device,), device_id_type=pl.DeviceIdType.MESH)
    pl.semaphore_wait(barrier, 3)
    rows, cols = out_ref.shape
    half = cols // 2
    left, right = pl.ds(0, half), pl.ds(half, half)

    def remote(i, src, dst, device):
        return pltpu.make_async_remote_copy(src_ref=src, dst_ref=dst, send_sem=send_sem.at[i], recv_sem=recv_sem.at[i], device_id=(device,), device_id_type=pl.DeviceIdType.MESH)

    def add(dst, *srcs):
        @pl.loop(0, rows // 32)
        def _(r):
            at = pl.ds(pl.multiple_of(r * 32, 32), 32)
            total = dst[at, :]
            for src in srcs:
                total = total + src[at, :]
            dst[at, :] = total

    order = (3, 1, 2, 0)
    pair = {j: remote(j, part_ref.at[peer_of(me, masks[j] + 1)], came.at[j], other) for j in order}
    local = {j: pltpu.make_async_copy(part_ref.at[peer_of(me, masks[j])], mine.at[j], local_sem.at[j]) for j in order}
    for j in order:
        pair[j].start()
        local[j].start()

    def summed(j):
        local[j].wait()
        pair[j].wait_recv()
        add(mine.at[j], came.at[j])

    far_a = remote(4, mine.at[3, :, left], first_a.at[1], across)
    far_b = remote(5, mine.at[3, :, right], first_b.at[1], along)
    near_a = remote(6, mine.at[1, :, left], first_a.at[0], across)
    near_b = remote(7, mine.at[2, :, right], first_b.at[0], along)
    next_a = remote(8, mine.at[2, :, left], last_a, along)
    next_b = remote(9, mine.at[1, :, right], last_b, across)
    summed(3)
    far_a.start()
    far_b.start()
    summed(1)
    near_a.start()
    summed(2)
    near_b.start()
    summed(0)
    far_a.wait_recv()
    add(mine.at[2, :, left], first_a.at[1])
    next_a.start()
    far_b.wait_recv()
    add(mine.at[1, :, right], first_b.at[1])
    next_b.start()
    near_a.wait_recv()
    add(mine.at[0, :, left], first_a.at[0])
    near_b.wait_recv()
    add(mine.at[0, :, right], first_b.at[0])

    def finish(where, extra):
        @pl.loop(0, rows // 32)
        def _(r):
            at = pl.ds(pl.multiple_of(r * 32, 32), 32)
            out_ref[at, where] = mine[0, at, where] + extra[at, :]

    next_a.wait_recv()
    finish(left, last_a)
    next_b.wait_recv()
    finish(right, last_b)
    for copy in (*pair.values(), far_a, far_b, near_a, near_b, next_a, next_b):
        copy.wait_send()


def reduce_blocks(part, collective_id):
    seq_len, cols = part.shape
    rows = seq_len // 8
    return pl.pallas_call(
        reduce_kernel,
        out_shape=jax.ShapeDtypeStruct((rows, cols), part.dtype),
        in_specs=[pl.BlockSpec(memory_space=pl.ANY)],
        out_specs=pl.BlockSpec(memory_space=pltpu.VMEM),
        scratch_shapes=[
            pltpu.VMEM((4, rows, cols), part.dtype),
            pltpu.VMEM((4, rows, cols), part.dtype),
            pltpu.VMEM((2, rows, cols // 2), part.dtype),
            pltpu.VMEM((2, rows, cols // 2), part.dtype),
            pltpu.VMEM((rows, cols // 2), part.dtype),
            pltpu.VMEM((rows, cols // 2), part.dtype),
            pltpu.SemaphoreType.DMA((10,)),
            pltpu.SemaphoreType.DMA((10,)),
            pltpu.SemaphoreType.DMA((4,)),
        ],
        compiler_params=pltpu.CompilerParams(collective_id=collective_id, has_side_effects=True, vmem_limit_bytes=40 * MIB),
        cost_estimate=cost(60000),
        name='reduce_blocks',
    )(part.reshape(8, rows, cols))


def swap_halves(values, head_dim):
    half = head_dim // 2
    lanes = values.shape[1]
    lane = lax.broadcasted_iota(jnp.int32, values.shape, 1)
    return jnp.where(lane % head_dim < half, pltpu.roll(values, lanes - half, 1), pltpu.roll(values, half, 1))


def rotate_lanes(values, cos_lanes, sin_lanes, head_dim):
    return values * cos_lanes + swap_halves(values, head_dim) * sin_lanes


def qkv_kernel(head_dim, me_ref, x_ref, gain_ref, w_ref, cos_ref, sin_ref, q_ref, k_ref, v_ref, u_rows_ref, x_rows_ref):
    width = q_ref.shape[1]
    hidden = x_ref[:].astype(F32)
    inv_rms = inverse_rms(hidden)
    normed = (hidden * inv_rms * gain_ref[:]).astype(B16)
    own = pl.ds(pl.multiple_of(me_ref[0] * u_rows_ref.shape[1], 128), u_rows_ref.shape[1])
    scaled = x_ref[:, own].astype(F32) * inv_rms
    x_rows_ref[:] = scaled
    u_rows_ref[:] = (scaled * gain_ref[:, own]).astype(B16)
    lin = jnp.dot(normed, w_ref[:], preferred_element_type=F32).astype(B16)
    cos_lanes, sin_lanes = cos_ref[:], sin_ref[:]
    rotated = [rotate_lanes(lin[:, i:i + 128].astype(F32), cos_lanes, sin_lanes, head_dim).astype(B16) for i in range(0, width + 128, 128)]
    q_ref[:] = jnp.concatenate(rotated[:-1], axis=1)
    k_ref[:] = rotated[-1][:, :head_dim]
    v_ref[:] = lin[:, width + head_dim:]


def project_qkv(me, x_full, gain, w_qkv, cos_lanes, sin_lanes, head_dim):
    seq_len, model_dim = x_full.shape
    width = w_qkv.shape[1] - 2 * head_dim
    part = BLOCK

    def tile(cols):
        return pl.BlockSpec((BLOCK, cols), lambda i, me_ref: (i, 0))

    return pl.pallas_call(
        functools.partial(qkv_kernel, head_dim),
        grid_spec=pltpu.PrefetchScalarGridSpec(
            num_scalar_prefetch=1,
            grid=(seq_len // BLOCK,),
            in_specs=[tile(model_dim), whole_block((1, model_dim)), whole_block(w_qkv.shape), tile(128), tile(128)],
            out_specs=(tile(width), tile(head_dim), tile(head_dim), tile(part), tile(part)),
        ),
        out_shape=(
            jax.ShapeDtypeStruct((seq_len, width), B16),
            jax.ShapeDtypeStruct((seq_len, head_dim), B16),
            jax.ShapeDtypeStruct((seq_len, head_dim), B16),
            jax.ShapeDtypeStruct((seq_len, part), B16),
            jax.ShapeDtypeStruct((seq_len, part), F32),
        ),
        compiler_params=pltpu.CompilerParams(vmem_limit_bytes=32 * MIB),
        cost_estimate=cost(3000),
        name='project_qkv',
    )(me.reshape(1), x_full, gain, w_qkv, cos_lanes, sin_lanes)


def hold_weights(me_ref, held_refs, block_refs):
    count = held_refs[0].shape[0]

    @pl.when(pl.program_id(0) == 0)
    def _():
        for i, held in enumerate(held_refs):
            for k, ref in zip((0,) + XOR_ORDER, block_refs[i * count:(i + 1) * count]):
                held[lax.bitwise_xor(me_ref[0], k)] = ref[0]

    return [held[:].reshape(count * held.shape[1], held.shape[2]) for held in held_refs]


def mlp_forward_kernel(me_ref, h_ref, gain_ref, down_ref, *refs):
    weight_refs, out_refs, held_refs = refs[:-7], refs[-7:-2], refs[-2:]
    m_ref, gate_ref, up_ref, glu_ref, y_ref = out_refs
    w_gate, w_up = hold_weights(me_ref, held_refs, weight_refs)
    hidden = h_ref[:].astype(F32)
    mlp_in = (hidden * inverse_rms(hidden) * gain_ref[:]).astype(B16)
    m_ref[:] = mlp_in
    gate_ref[:] = gate = jnp.dot(mlp_in, w_gate, preferred_element_type=F32).astype(B16)
    up_ref[:] = up = jnp.dot(mlp_in, w_up, preferred_element_type=F32).astype(B16)
    glu_ref[:] = glu = gated_unit(gate.astype(F32), up.astype(F32)).astype(B16)
    y_ref[:] = jnp.dot(glu, down_ref[:], preferred_element_type=F32)


def mlp_backward_kernel(me_ref, gate_ref, up_ref, dy_ref, down_ref, *refs):
    weight_refs, (da_ref, db_ref, dm_ref), held_refs = refs[:-5], refs[-5:-2], refs[-2:]
    w_gate, w_up = hold_weights(me_ref, held_refs, weight_refs)
    gate, up = gate_ref[:].astype(F32), up_ref[:].astype(F32)
    d_glu = dot_f32(dy_ref[:], down_ref[:], ((1,), (1,))).astype(B16).astype(F32)
    sig = jax.nn.sigmoid(gate)
    silu = gate * sig
    da_ref[:] = d_gate = (d_glu * up * (sig + silu * (1.0 - sig))).astype(B16)
    db_ref[:] = d_up = (d_glu * silu).astype(B16)
    dm_ref[:] = dot_f32(d_gate, w_gate, ((1,), (1,))) + dot_f32(d_up, w_up, ((1,), (1,)))


def token_tile(cols):
    return pl.BlockSpec((MLP_BLOCK, cols), lambda i, me_ref: (i, 0))


def whole_block(shape):
    return pl.BlockSpec(shape, lambda *ids: (0,) * len(shape))


def mlp_call(kernel, me, operands, operand_specs, weights, out_cols, out_types, flops):
    seq_len = operands[0].shape[0]
    count, rows, part = weights[0].shape
    own_spec = pl.BlockSpec((1, rows, part), lambda i, me_ref: (me_ref[0], 0, 0))
    came_spec = whole_block((1, rows, part))
    weight_specs = ([own_spec] + [came_spec] * (count - 1)) * 2
    return pl.pallas_call(
        kernel,
        grid_spec=pltpu.PrefetchScalarGridSpec(
            num_scalar_prefetch=1,
            grid=(seq_len // MLP_BLOCK,),
            in_specs=operand_specs + weight_specs,
            out_specs=tuple(token_tile(cols) for cols in out_cols),
            scratch_shapes=[pltpu.VMEM((count, rows, part), B16), pltpu.VMEM((count, rows, part), B16)],
        ),
        out_shape=tuple(jax.ShapeDtypeStruct((seq_len, cols), dtype) for cols, dtype in zip(out_cols, out_types)),
        compiler_params=pltpu.CompilerParams(vmem_limit_bytes=60 * MIB),
        cost_estimate=cost(flops),
    )(me.reshape(1), *operands, *weights)


def ffn_grad_kernel(me_ref, m_ref, da_ref, db_ref, *refs):
    out_refs, (da_t, db_t) = refs[:-2], refs[-2:]
    count = len(out_refs) // 2
    step = pl.program_id(0)

    @pl.when(step == 0)
    def _():
        da_t[:] = da_ref[:].T
        db_t[:] = db_ref[:].T

    for k in range(count):
        @pl.when(step == k)
        def _():
            out_refs[k][0] = jnp.dot(da_t[:], m_ref[:], preferred_element_type=F32)
            out_refs[count + k][0] = jnp.dot(db_t[:], m_ref[:], preferred_element_type=F32)


def ffn_grads(me, mlp_in, d_gate_act, d_up_act, count):
    seq_len, model_dim = mlp_in.shape
    rows, part = model_dim // count, d_gate_act.shape[1]
    shape = jax.ShapeDtypeStruct((1, part, rows), F32)
    blocks = pl.pallas_call(
        ffn_grad_kernel,
        grid_spec=pltpu.PrefetchScalarGridSpec(
            num_scalar_prefetch=1,
            grid=(count,),
            in_specs=[pl.BlockSpec((seq_len, rows), lambda k, me_ref: (0, lax.bitwise_xor(me_ref[0], k)))] + [whole_block((seq_len, part))] * 2,
            out_specs=(whole_block(shape.shape),) * (2 * count),
            scratch_shapes=[pltpu.VMEM((part, seq_len), B16), pltpu.VMEM((part, seq_len), B16)],
        ),
        out_shape=(shape,) * (2 * count),
        compiler_params=pltpu.CompilerParams(vmem_limit_bytes=56 * MIB),
        cost_estimate=cost(12000),
        name='ffn_grads',
    )(me.reshape(1), mlp_in, d_gate_act, d_up_act)
    return blocks[:count], blocks[count:]


def join_kernel(me_ref, *refs):
    blocks, out_ref, held = refs[:-2], refs[-2], refs[-1]
    for k, ref in zip((0,) + XOR_ORDER, blocks):
        held[lax.bitwise_xor(me_ref[0], k)] = ref[0]
    count, width, rows = held.shape
    for pair in range(count // 2):
        out_ref[:, pair * 2 * width:(pair + 1) * 2 * width] = held[2 * pair:2 * pair + 2].reshape(2 * width, rows).T


def join_columns(me, own, came):
    count = 1 + len(came)
    width, rows = own.shape[1:]
    tile = 128
    spec = pl.BlockSpec((1, width, tile), lambda i, me_ref: (0, 0, i))
    return pl.pallas_call(
        join_kernel,
        grid_spec=pltpu.PrefetchScalarGridSpec(
            num_scalar_prefetch=1,
            grid=(rows // tile,),
            in_specs=[spec] * count,
            out_specs=pl.BlockSpec((tile, count * width), lambda i, me_ref: (i, 0)),
            scratch_shapes=[pltpu.VMEM((count, width, tile), own.dtype)],
        ),
        out_shape=jax.ShapeDtypeStruct((rows, count * width), own.dtype),
        compiler_params=pltpu.CompilerParams(vmem_limit_bytes=32 * MIB),
        cost_estimate=cost(1),
        name='join_columns',
    )(me.reshape(1), own, *came)


def pair_heads_kernel(k_ref, v_ref, out_ref):
    width = k_ref.shape[1] // 4
    parts = [ref[:, h * width:(h + 1) * width] for h in range(4) for ref in (k_ref, v_ref)]
    out_ref[:] = jnp.concatenate(parts, axis=1)


def pair_heads(wk_rows, wv_rows):
    rows, cols = wk_rows.shape
    return pl.pallas_call(pair_heads_kernel, out_shape=jax.ShapeDtypeStruct((rows, 2 * cols), B16), name='pair_heads')(wk_rows, wv_rows)


def normed_grad_kernel(width, head_dim, g_ref, x_ref, wq_ref, wkv_ref, cos_ref, sin_ref, dkv_ref, du_ref, dg_ref, acc_ref, share_ref):
    step = pl.program_id(0)
    half = head_dim // 2

    @pl.when(step == 0)
    def _():
        acc_ref[:] = jnp.zeros_like(acc_ref)

    acc_ref[:] += jnp.dot(wq_ref[:], g_ref[0, :width, :], preferred_element_type=F32)
    share = g_ref[0, width:width + 2 * head_dim, :].astype(F32)

    @pl.when(step % 2 == 0)
    def _():
        share_ref[:] = share

    @pl.when(step % 2 == 1)
    def _():
        summed = (share_ref[:] + share).astype(B16)
        first, second = summed[:half].astype(F32), summed[half:head_dim].astype(F32)
        cos_rows, sin_rows = cos_ref[:], sin_ref[:]
        dk = jnp.concatenate([first * cos_rows + second * sin_rows, second * cos_rows - first * sin_rows], axis=0).astype(B16)
        dkv = jnp.concatenate([dk, summed[head_dim:]], axis=0)
        dkv_ref[0] = dkv
        acc_ref[:] += jnp.dot(wkv_ref[:], dkv, preferred_element_type=F32)

    @pl.when(step == pl.num_programs(0) - 1)
    def _():
        d_normed = acc_ref[:].T.astype(B16)
        du_ref[:] = d_normed
        dg_ref[:] = jnp.sum(d_normed.astype(F32) * x_ref[:], axis=0, keepdims=True)


def normed_grads(gathered, x_rows, wq_rows, wkv_rows, cos_t, sin_t, head_dim):
    count, height, seq_len = gathered.shape
    rows = x_rows.shape[1]
    width = wq_rows.shape[1] // count

    return pl.pallas_call(
        functools.partial(normed_grad_kernel, width, head_dim),
        grid=(count,),
        in_specs=[
            pl.BlockSpec((1, height, seq_len), lambda e: (e, 0, 0)),
            whole_block(x_rows.shape),
            pl.BlockSpec((rows, width), lambda e: (0, e)),
            pl.BlockSpec((rows, 2 * head_dim), lambda e: (0, e // 2)),
            whole_block(cos_t.shape),
            whole_block(sin_t.shape),
        ],
        out_specs=(pl.BlockSpec((1, 2 * head_dim, seq_len), lambda e: (e // 2, 0, 0)), whole_block((seq_len, rows)), whole_block((1, rows))),
        out_shape=(
            jax.ShapeDtypeStruct((count // 2, 2 * head_dim, seq_len), B16),
            jax.ShapeDtypeStruct((seq_len, rows), B16),
            jax.ShapeDtypeStruct((1, rows), F32),
        ),
        scratch_shapes=[pltpu.VMEM((rows, seq_len), F32), pltpu.VMEM((2 * head_dim, seq_len), F32)],
        compiler_params=pltpu.CompilerParams(vmem_limit_bytes=40 * MIB),
        cost_estimate=cost(3000),
        name='normed_grads',
    )(gathered, x_rows, wq_rows, wkv_rows, cos_t, sin_t)


def qkv_grad_kernel(width, head_dim, g_ref, dkv_ref, u_ref, dwq_ref, dwk_ref, dwv_ref):
    step = pl.program_id(0)
    dwq_ref[:] = jnp.dot(g_ref[0, :width, :], u_ref[:], preferred_element_type=F32).T
    kv_heads = dkv_ref.shape[0]

    @pl.when(step == 0)
    def _():
        both = jnp.dot(dkv_ref[:].reshape(kv_heads * 2 * head_dim, -1), u_ref[:], preferred_element_type=F32).T
        for out_ref, offset in ((dwk_ref, 0), (dwv_ref, head_dim)):
            out_ref[:] = jnp.concatenate([both[:, h * 2 * head_dim + offset:h * 2 * head_dim + offset + head_dim] for h in range(kv_heads)], axis=1)


def qkv_grads(gathered, dkv_t, u_rows, width, head_dim):
    count, height, seq_len = gathered.shape
    rows = u_rows.shape[1]
    kv_width = dkv_t.shape[0] * head_dim
    kv_spec = whole_block((rows, kv_width))
    return pl.pallas_call(
        functools.partial(qkv_grad_kernel, width, head_dim),
        grid=(count,),
        in_specs=[
            pl.BlockSpec((1, height, seq_len), lambda e: (e, 0, 0)),
            whole_block(dkv_t.shape),
            whole_block(u_rows.shape),
        ],
        out_specs=(pl.BlockSpec((rows, width), lambda e: (0, e)), kv_spec, kv_spec),
        out_shape=(
            jax.ShapeDtypeStruct((rows, count * width), F32),
            jax.ShapeDtypeStruct((rows, kv_width), F32),
            jax.ShapeDtypeStruct((rows, kv_width), F32),
        ),
        compiler_params=pltpu.CompilerParams(vmem_limit_bytes=40 * MIB),
        cost_estimate=cost(3000),
        name='qkv_grads',
    )(gathered, dkv_t, u_rows)


def solution(mesh):
    n_dev = mesh.shape['sp']
    gather_rows = functools.partial(lax.all_gather, axis_name='sp', axis=0, tiled=True)
    scatter_rows = functools.partial(lax.psum_scatter, axis_name='sp', scatter_dimension=0, tiled=True)
    swap_blocks = functools.partial(lax.all_to_all, axis_name='sp', split_axis=0, concat_axis=0, tiled=True)

    def send_blocks(others, order=XOR_ORDER):
        others = lax.optimization_barrier(tuple(with_layout_constraint(other, Layout((0, 1, 2))) for other in others))
        came = []
        for k, other in zip(order, others):
            came.append(with_layout_constraint(lax.ppermute(other, 'sp', [(i, i ^ k) for i in range(n_dev)]), Layout((0, 1, 2))))
        return came

    def pick_blocks(blocks):
        me = lax.axis_index('sp')
        return [lax.dynamic_index_in_dim(blocks, lax.bitwise_xor(me, k), axis=0, keepdims=True) for k in XOR_ORDER]

    def after(value, *others):
        return lax.optimization_barrier((value,) + others)[0]

    def to_tokens(columns):
        blocks = swap_blocks(columns.reshape(n_dev, -1, columns.shape[1]))
        return blocks.transpose(1, 0, 2).reshape(blocks.shape[1], -1)

    def layer_step(x_in, positions, d_out, norm1_gain, norm2_gain, w_q, w_k, w_v, w_o, w_gate, w_up, w_down):
        tokens, model_dim = x_in.shape
        rows = model_dim // n_dev
        seq_len = tokens * n_dev
        q_heads, head_dim = w_q.shape[1:]
        kv_heads = w_k.shape[1]
        heads = q_heads // n_dev
        width = heads * head_dim
        kv_repeat = n_dev // kv_heads
        ffn_part = w_down.shape[0]
        me = lax.axis_index('sp')
        own_rows = functools.partial(lax.dynamic_slice_in_dim, start_index=me * rows, slice_size=rows, axis=1)

        x_full = gather_rows(x_in)
        wq_rows = w_q.reshape(rows, q_heads * head_dim)
        wk_rows = w_k.reshape(rows, kv_heads * head_dim)
        wv_rows = w_v.reshape(rows, kv_heads * head_dim)
        wo_rows = w_o.reshape(width, model_dim)

        wq_blocks = wq_rows.reshape(rows, n_dev, width).transpose(1, 0, 2)
        wk_blocks = jnp.repeat(w_k.transpose(1, 0, 2), kv_repeat, axis=0)
        wv_blocks = jnp.repeat(w_v.transpose(1, 0, 2), kv_repeat, axis=0)
        qkv_blocks = jnp.concatenate([wq_blocks, wk_blocks, wv_blocks], axis=2)
        lane_width = qkv_blocks.shape[2]
        small = jnp.stack([norm1_gain, norm2_gain, (positions // 128).astype(B16), (positions % 128).astype(B16)])
        small = jnp.pad(small, ((0, 12), (0, lane_width - rows)))
        small = jnp.broadcast_to(small[None], (n_dev,) + small.shape)
        qkv_cols = swap_blocks(jnp.concatenate([qkv_blocks, small], axis=1))
        w_qkv = qkv_cols[:, :rows].reshape(model_dim, lane_width)
        gain1 = qkv_cols[:, rows, :rows].reshape(model_dim).astype(F32)
        gain2 = qkv_cols[:, rows + 1, :rows].reshape(model_dim).astype(F32)
        pos_all = (qkv_cols[:, rows + 2, :rows].astype(F32) * 128.0 + qkv_cols[:, rows + 3, :rows].astype(F32)).reshape(seq_len)

        wo_full = gather_rows(wo_rows)
        dy_full = gather_rows(d_out)
        gate_blocks = w_gate.reshape(rows, n_dev, ffn_part).transpose(1, 0, 2)
        up_blocks = w_up.reshape(rows, n_dev, ffn_part).transpose(1, 0, 2)
        gate_others, up_others = pick_blocks(gate_blocks), pick_blocks(up_blocks)
        gate_came = send_blocks(gate_others[:FIRST], XOR_ORDER[:FIRST])
        gate_others, up_others, x_full = lax.optimization_barrier((gate_others[FIRST:], up_others, x_full))
        gate_came, up_came = gate_came + send_blocks(gate_others, XOR_ORDER[FIRST:]), send_blocks(up_others)

        cos_tab, sin_tab = rope_tables(pos_all, head_dim)
        cos_tab, sin_tab = cos_tab[:, 0], sin_tab[:, 0]
        cos_lanes = jnp.tile(cos_tab, (1, 4))
        sin_lanes = jnp.tile(jnp.concatenate([-sin_tab, sin_tab], axis=1), (1, 2))
        q_rot, k_rot, v_lin, u_rows, x_rows = project_qkv(me, x_full, gain1[None], w_qkv, cos_lanes, sin_lanes, head_dim)
        attn_cols, row_max, inv_sum = attention_forward(q_rot, k_rot, v_lin, heads)
        attn_tok = to_tokens(attn_cols)
        hidden = (x_in.astype(F32) + jnp.dot(attn_tok, wo_full, preferred_element_type=F32)).astype(B16)
        h_full = gather_blocks(hidden, 1)
        wk_late, wv_late = lax.optimization_barrier((wk_rows, wv_rows, hidden))[:2]
        wkv_rows = pair_heads(wk_late, wv_late)
        weights = (gate_blocks, *gate_came, up_blocks, *up_came)
        mlp_in, gate_act, up_act, glu_out, y_part = mlp_call(
            mlp_forward_kernel, me, (h_full, gain2[None], w_down),
            [token_tile(model_dim), whole_block((1, model_dim)), whole_block(w_down.shape)],
            weights, (model_dim, ffn_part, ffn_part, ffn_part, model_dim), (B16, B16, B16, B16, F32), 18_000)
        y_sum = scatter_rows(y_part)
        d_gate_act, d_up_act, d_mlp_part = mlp_call(
            mlp_backward_kernel, me, (gate_act, up_act, dy_full, w_down),
            [token_tile(ffn_part), token_tile(ffn_part), token_tile(model_dim), whole_block(w_down.shape)],
            weights, (ffn_part, ffn_part, model_dim), (B16, B16, F32), 18_000)
        d_gate_blocks, d_up_blocks = ffn_grads(me, mlp_in, d_gate_act, d_up_act, n_dev)
        d_gate_others = [d_gate_blocks[k] for k in XOR_ORDER]
        d_up_others = [d_up_blocks[k] for k in XOR_ORDER]
        cos_t, sin_t = cos_tab.T, sin_tab.T
        d_mlp_part, d_up_others, d_gate_others, cos_t, sin_t, wkv_rows = lax.optimization_barrier((d_mlp_part, d_up_others, d_gate_others, cos_t, sin_t, wkv_rows))
        d_gate_came = send_blocks(d_gate_others[:NOW], XOR_ORDER[:NOW])
        d_mlp_sum = reduce_blocks(d_mlp_part, 4)
        d_mlp_in = d_mlp_sum.astype(B16).astype(F32)
        hidden_f = hidden.astype(F32)
        inv2 = inverse_rms(hidden_f)
        d_hidden = (d_out.astype(F32) + norm_backward(d_mlp_in, hidden_f, inv2, gain2)).astype(B16)
        d_g2_part = jnp.sum(d_mlp_in * hidden_f * inv2, axis=0)
        dh_full = gather_blocks(d_hidden, 2)
        d_gate_came += send_blocks(after(d_gate_others[NOW:], dh_full), XOR_ORDER[NOW:])
        d_up_came = send_blocks(after(d_up_others[:EARLY], dh_full), XOR_ORDER[:EARLY])

        d_attn = jnp.einsum('td,cd->tc', dh_full, wo_rows, preferred_element_type=F32).astype(B16)
        dq_t, dk_t, dv_t = attention_backward(q_rot, d_attn, k_rot, v_lin, row_max, inv_sum, cos_lanes, sin_lanes, heads)
        piece_hi = lax.reduce_precision(d_g2_part, 8, 7)
        piece_mid = lax.reduce_precision(d_g2_part - piece_hi, 8, 7)
        piece_lo = lax.reduce_precision(d_g2_part - piece_hi - piece_mid, 8, 7)
        pieces = jnp.pad(jnp.stack([piece_hi, piece_mid, piece_lo]).astype(B16), ((0, 13), (0, 0)))
        dqkv_t = gather_rows(jnp.concatenate([dq_t, dk_t, dv_t, pieces], axis=0)).reshape(n_dev, width + 2 * head_dim + 16, seq_len)
        d_g2 = jnp.sum(own_rows(dqkv_t[:, width + 2 * head_dim:width + 2 * head_dim + 3].reshape(-1, seq_len)).astype(F32), axis=0)
        glu_late, o_late = lax.optimization_barrier((glu_out, attn_cols, dk_t))[:2]
        d_down = jnp.einsum('tf,td->fd', glu_late, dy_full, preferred_element_type=F32)
        d_wo = jnp.einsum('tc,td->cd', o_late, dh_full, preferred_element_type=F32)
        d_gate = join_columns(me, d_gate_blocks[0], d_gate_came)
        dqkv_t, d_down, d_wo, d_gate = lax.optimization_barrier((dqkv_t, d_down, d_wo, d_gate))
        d_up_came += send_blocks(after(d_up_others[EARLY:], dqkv_t), XOR_ORDER[EARLY:])
        d_up = join_columns(me, d_up_blocks[0], d_up_came)
        y_out = (hidden_f + y_sum).astype(B16)

        dkv_t, d_norm_cols, d_g1 = normed_grads(dqkv_t, x_rows, wq_rows, wkv_rows, cos_t, sin_t, head_dim)
        d_wq, d_wk, d_wv = qkv_grads(dqkv_t, dkv_t, u_rows, width, head_dim)
        d_g1 = d_g1[0]
        d_normed = to_tokens(d_norm_cols).astype(F32)
        x_f32 = x_in.astype(F32)
        d_x = (d_hidden.astype(F32) + norm_backward(d_normed, x_f32, inverse_rms(x_f32), gain1)).astype(B16)
        return (y_out, d_x, d_g1, d_g2, d_wq.reshape(w_q.shape), d_wk.reshape(w_k.shape), d_wv.reshape(w_v.shape), d_wo.reshape(w_o.shape), d_gate, d_up, d_down)

    all_rows = P('sp')
    return jax.shard_map(layer_step, mesh=mesh, in_specs=(all_rows,) * 12, out_specs=(all_rows,) * 11, check_vma=False)
```

```python
import functools
import jax
import jax.numpy as jnp
from jax import lax
from jax.experimental import pallas as pl
from jax.experimental.pallas import tpu as pltpu
from jax.experimental.layout import Layout, with_layout_constraint
from jax.sharding import PartitionSpec as P

ROPE_BASE = 10000.0
NORM_EPS = 1e-5
NEG_LARGE = -1e30
BLOCK = 256
MLP_BLOCK = 256
MIB = 1024 * 1024
EARLY = 3
NOW = 3
FIRST = 2
XOR_ORDER = (2, 4, 6, 3, 5, 7, 1)
B16 = jnp.bfloat16
F32 = jnp.float32


def inverse_rms(hidden):
    return lax.rsqrt(jnp.mean(hidden * hidden, axis=-1, keepdims=True) + NORM_EPS)


def rope_tables(positions, head_dim):
    half_dim = head_dim // 2
    inv_freq = 1.0 / (ROPE_BASE ** (jnp.arange(half_dim, dtype=F32) * (2.0 / head_dim)))
    angles = positions.astype(F32)[:, None] * inv_freq[None, :]
    return jnp.cos(angles)[:, None, :], jnp.sin(angles)[:, None, :]


def cost(mega_flops):
    return pl.CostEstimate(flops=mega_flops * 1_000_000, bytes_accessed=20_000_000, transcendentals=0)


def gated_unit(gate_pre, up_pre):
    return jax.nn.silu(gate_pre) * up_pre


def norm_backward(d_normed, hidden, inv_rms, gain):
    scaled = d_normed * gain
    row_dot = jnp.mean(scaled * hidden, axis=-1, keepdims=True)
    return inv_rms * scaled - hidden * (inv_rms * inv_rms * inv_rms * row_dot)


def stack_heads(block, heads, head_dim):
    return jnp.concatenate([block[:, h * head_dim:(h + 1) * head_dim] for h in range(heads)], axis=0)


def unstack_heads(rows, heads):
    size = rows.shape[0] // heads
    return jnp.concatenate([rows[h * size:(h + 1) * size] for h in range(heads)], axis=1)


def dot_f32(lhs, rhs, dims):
    return lax.dot_general(lhs, rhs, (dims, ((), ())), preferred_element_type=F32)


def causal_block(heads):
    shape = (heads * BLOCK, BLOCK)
    row = lax.broadcasted_iota(jnp.int32, shape, 0) % BLOCK
    col = lax.broadcasted_iota(jnp.int32, shape, 1)
    return row >= col


def attention_forward_kernel(heads, head_dim, scale, q_ref, k_ref, v_ref, o_ref, max_ref, inv_ref, score_ref, acc_ref):
    step = pl.program_id(0)
    queries = stack_heads(q_ref[:], heads, head_dim)
    last = pl.multiple_of(step * BLOCK, BLOCK)

    def scores_at(start):
        return dot_f32(queries, k_ref[pl.ds(start, BLOCK), :], ((1,), (1,))) * scale

    def fold(op, block):
        return op(block[:, :128], block[:, 128:])

    diag = jnp.where(causal_block(heads), scores_at(last), NEG_LARGE)
    score_ref[:, pl.ds(last, BLOCK)] = diag
    acc_ref[:] = fold(jnp.maximum, diag)

    @pl.loop(0, step)
    def _(j):
        start = pl.multiple_of(j * BLOCK, BLOCK)
        block = scores_at(start)
        score_ref[:, pl.ds(start, BLOCK)] = block
        acc_ref[:] = jnp.maximum(acc_ref[:], fold(jnp.maximum, block))

    row_max = jnp.max(acc_ref[:], axis=1, keepdims=True)
    max_ref[:] = row_max
    acc_ref[:] = jnp.zeros_like(acc_ref)

    @pl.loop(0, step + 1)
    def _(j):
        start = pl.multiple_of(j * BLOCK, BLOCK)
        block = jnp.exp(score_ref[:, pl.ds(start, BLOCK)] - row_max)
        score_ref[:, pl.ds(start, BLOCK)] = block
        acc_ref[:] += fold(jnp.add, block)

    inv_sum = 1.0 / jnp.sum(acc_ref[:], axis=1, keepdims=True)
    inv_ref[:] = inv_sum

    def weighted(j, total):
        start = pl.multiple_of(j * BLOCK, BLOCK)
        probs = (score_ref[:, pl.ds(start, BLOCK)] * inv_sum).astype(B16)
        return total + dot_f32(probs, v_ref[pl.ds(start, BLOCK), :], ((1,), (0,)))

    total = lax.fori_loop(0, step + 1, weighted, jnp.zeros((heads * BLOCK, head_dim), F32))
    o_ref[:] = unstack_heads(total.astype(B16), heads)


def attention_forward(q_rot, k_rot, v_lin, heads):
    seq_len, width = q_rot.shape
    head_dim = width // heads
    rows = heads * BLOCK
    steps = seq_len // BLOCK
    whole = whole_block((seq_len, head_dim))
    tokens = pl.BlockSpec((BLOCK, width), lambda i: (i, 0))
    stats = pl.BlockSpec((rows, 1), lambda i: (i, 0))
    stat_shape = jax.ShapeDtypeStruct((steps * rows, 1), F32)
    return pl.pallas_call(
        functools.partial(attention_forward_kernel, heads, head_dim, head_dim ** -0.5),
        grid=(steps,),
        out_shape=(jax.ShapeDtypeStruct((seq_len, width), B16), stat_shape, stat_shape),
        in_specs=[tokens, whole, whole],
        out_specs=(tokens, stats, stats),
        scratch_shapes=[pltpu.VMEM((rows, seq_len), F32), pltpu.VMEM((rows, 128), F32)],
        compiler_params=pltpu.CompilerParams(vmem_limit_bytes=48 * MIB),
        cost_estimate=cost(20000),
        name='attention_forward',
    )(q_rot, k_rot, v_lin)


def attention_backward_kernel(heads, head_dim, scale, q_ref, do_ref, k_ref, v_ref, max_ref, inv_ref, cos_ref, sin_ref, dq_ref, dk_ref, dv_ref, prob_ref, dp_ref, acc_ref, dk_acc, dv_acc):
    step = pl.program_id(0)
    queries = stack_heads(q_ref[:], heads, head_dim)
    d_out = stack_heads(do_ref[:], heads, head_dim)
    row_max = max_ref[:]
    inv_sum = inv_ref[:]
    last = pl.multiple_of(step * BLOCK, BLOCK)

    @pl.when(step == 0)
    def _():
        dk_acc[:] = jnp.zeros_like(dk_acc)
        dv_acc[:] = jnp.zeros_like(dv_acc)

    def scores_at(start):
        return dot_f32(queries, k_ref[pl.ds(start, BLOCK), :], ((1,), (1,))) * scale

    def first_pass(start, scores):
        probs = jnp.exp(scores - row_max) * inv_sum
        d_probs = dot_f32(d_out, v_ref[pl.ds(start, BLOCK), :], ((1,), (1,))).astype(B16)
        prob_ref[:, pl.ds(start, BLOCK)] = probs
        dp_ref[:, pl.ds(start, BLOCK)] = d_probs
        product = probs * d_probs.astype(F32)
        dv_acc[:, pl.ds(start, BLOCK)] += dot_f32(d_out, probs.astype(B16), ((0,), (0,)))
        return product[:, :128] + product[:, 128:]

    acc_ref[:] = first_pass(last, jnp.where(causal_block(heads), scores_at(last), NEG_LARGE))

    @pl.loop(0, step)
    def _(j):
        start = pl.multiple_of(j * BLOCK, BLOCK)
        acc_ref[:] += first_pass(start, scores_at(start))

    row_dot = jnp.sum(acc_ref[:], axis=1, keepdims=True)

    def second_pass(j, total):
        start = pl.multiple_of(j * BLOCK, BLOCK)
        at = pl.ds(start, BLOCK)
        d_scores = (prob_ref[:, at] * (dp_ref[:, at].astype(F32) - row_dot) * scale).astype(B16)
        dk_acc[:, at] += dot_f32(queries, d_scores, ((0,), (0,)))
        return total + dot_f32(d_scores, k_ref[at, :], ((1,), (0,)))

    total = lax.fori_loop(0, step + 1, second_pass, jnp.zeros((heads * BLOCK, head_dim), F32))
    d_rot = unstack_heads(total.astype(B16), heads).astype(F32)
    cos_lanes, sin_lanes = cos_ref[:], sin_ref[:]
    d_lin = [rotate_lanes(d_rot[:, i:i + 128], cos_lanes, -sin_lanes, head_dim) for i in range(0, heads * head_dim, 128)]
    dq_ref[:] = jnp.concatenate(d_lin, axis=1).T.astype(B16)

    @pl.when(step == pl.num_programs(0) - 1)
    def _():
        dk_ref[:] = dk_acc[:].astype(B16)
        dv_ref[:] = dv_acc[:].astype(B16)


def attention_backward(q_rot, d_attn, k_rot, v_lin, row_max, inv_sum, cos_lanes, sin_lanes, heads):
    seq_len, width = q_rot.shape
    head_dim = width // heads
    rows = heads * BLOCK
    steps = seq_len // BLOCK
    whole = whole_block((seq_len, head_dim))
    whole_t = whole_block((head_dim, seq_len))
    tokens = pl.BlockSpec((BLOCK, width), lambda i: (i, 0))
    stats = pl.BlockSpec((rows, 1), lambda i: (i, 0))
    grad_t = jax.ShapeDtypeStruct((head_dim, seq_len), B16)
    table = pl.BlockSpec((BLOCK, 128), lambda i: (i, 0))
    return pl.pallas_call(
        functools.partial(attention_backward_kernel, heads, head_dim, head_dim ** -0.5),
        grid=(steps,),
        out_shape=(jax.ShapeDtypeStruct((width, seq_len), B16), grad_t, grad_t),
        in_specs=[tokens, tokens, whole, whole, stats, stats, table, table],
        out_specs=(pl.BlockSpec((width, BLOCK), lambda i: (0, i)), whole_t, whole_t),
        scratch_shapes=[
            pltpu.VMEM((rows, seq_len), F32),
            pltpu.VMEM((rows, seq_len), B16),
            pltpu.VMEM((rows, 128), F32),
            pltpu.VMEM((head_dim, seq_len), F32),
            pltpu.VMEM((head_dim, seq_len), F32),
        ],
        compiler_params=pltpu.CompilerParams(vmem_limit_bytes=48 * MIB),
        cost_estimate=cost(40000),
        name='attention_backward',
    )(q_rot, d_attn, k_rot, v_lin, row_max, inv_sum, cos_lanes, sin_lanes)


def peer_of(me, mask):
    result = 0
    for bit in (1, 2, 4):
        mine = lax.rem(me // bit, 2)
        result = result + bit * ((1 - mine) if mask & bit else mine)
    return result


def gather_kernel(split, src_ref, out_ref, send_sem, recv_sem, local_sem):
    me = lax.axis_index('sp')
    rows = src_ref.shape[0]
    across, along, other, diagonal = (peer_of(me, mask) for mask in (2, 4, 1, 6))
    barrier = pltpu.get_barrier_semaphore()
    for device in (across, along, other):
        pl.semaphore_signal(barrier, inc=1, device_id=(device,), device_id_type=pl.DeviceIdType.MESH)
    pl.semaphore_wait(barrier, 3)

    upper, lower = (0, split), (split, rows - split)

    def place(owner, part):
        return out_ref.at[pl.ds(pl.multiple_of(owner * rows + part[0], 16), part[1]), :]

    def own(part):
        return src_ref.at[pl.ds(part[0], part[1]), :]

    plan = [
        (own(upper), place(me, upper), along),
        (own(lower), place(me, lower), across),
        (own(lower), place(me, lower), along),
        (own(upper), place(me, upper), across),
        (own((0, rows)), place(me, (0, rows)), other),
        (place(along, upper), place(along, upper), across),
        (place(across, lower), place(across, lower), along),
        (place(along, upper), place(along, upper), other),
        (place(across, lower), place(across, lower), other),
        (place(along, lower), place(along, lower), other),
        (place(across, upper), place(across, upper), other),
        (place(diagonal, upper), place(diagonal, upper), other),
        (place(diagonal, lower), place(diagonal, lower), other),
    ]
    copies = [
        pltpu.make_async_remote_copy(src_ref=src, dst_ref=dst, send_sem=send_sem.at[i], recv_sem=recv_sem.at[i], device_id=(device,), device_id_type=pl.DeviceIdType.MESH)
        for i, (src, dst, device) in enumerate(plan)
    ]
    for i in range(5):
        copies[i].start()
    mine = pltpu.make_async_copy(src_ref, place(me, (0, rows)), local_sem)
    mine.start()
    for came, go in ((0, (5, 7)), (1, (6, 8)), (2, (9,)), (3, (10,)), (5, (11,)), (6, (12,))):
        copies[came].wait_recv()
        for i in go:
            copies[i].start()
    for i in (4, 7, 8, 9, 10, 11, 12):
        copies[i].wait_recv()
    for copy in copies:
        copy.wait_send()
    mine.wait()


def gather_blocks(block, collective_id):
    rows, cols = block.shape
    split = (rows // 2 + 15) // 16 * 16
    return pl.pallas_call(
        functools.partial(gather_kernel, split),
        out_shape=jax.ShapeDtypeStruct((8 * rows, cols), block.dtype),
        in_specs=[pl.BlockSpec(memory_space=pltpu.VMEM)],
        out_specs=pl.BlockSpec(memory_space=pl.ANY),
        scratch_shapes=[pltpu.SemaphoreType.DMA((13,)), pltpu.SemaphoreType.DMA((13,)), pltpu.SemaphoreType.DMA],
        compiler_params=pltpu.CompilerParams(collective_id=collective_id, has_side_effects=True),
        cost_estimate=cost(30000),
        name='gather_blocks',
    )(block)


def reduce_kernel(part_ref, out_ref, mine, came, first_a, first_b, last_a, last_b, send_sem, recv_sem, local_sem):
    me = lax.axis_index('sp')
    masks = (0, 2, 4, 6)
    across, along, other = (peer_of(me, mask) for mask in (2, 4, 1))
    barrier = pltpu.get_barrier_semaphore()
    for device in (across, along, other):
        pl.semaphore_signal(barrier, inc=1, device_id=(device,), device_id_type=pl.DeviceIdType.MESH)
    pl.semaphore_wait(barrier, 3)
    rows, cols = out_ref.shape
    half = cols // 2
    left, right = pl.ds(0, half), pl.ds(half, half)

    def remote(i, src, dst, device):
        return pltpu.make_async_remote_copy(src_ref=src, dst_ref=dst, send_sem=send_sem.at[i], recv_sem=recv_sem.at[i], device_id=(device,), device_id_type=pl.DeviceIdType.MESH)

    def add(dst, *srcs):
        @pl.loop(0, rows // 32)
        def _(r):
            at = pl.ds(pl.multiple_of(r * 32, 32), 32)
            total = dst[at, :]
            for src in srcs:
                total = total + src[at, :]
            dst[at, :] = total

    order = (3, 1, 2, 0)
    pair = {j: remote(j, part_ref.at[peer_of(me, masks[j] + 1)], came.at[j], other) for j in order}
    local = {j: pltpu.make_async_copy(part_ref.at[peer_of(me, masks[j])], mine.at[j], local_sem.at[j]) for j in order}
    for j in order:
        pair[j].start()
        local[j].start()

    def summed(j):
        local[j].wait()
        pair[j].wait_recv()
        add(mine.at[j], came.at[j])

    far_a = remote(4, mine.at[3, :, left], first_a.at[1], across)
    far_b = remote(5, mine.at[3, :, right], first_b.at[1], along)
    near_a = remote(6, mine.at[1, :, left], first_a.at[0], across)
    near_b = remote(7, mine.at[2, :, right], first_b.at[0], along)
    next_a = remote(8, mine.at[2, :, left], last_a, along)
    next_b = remote(9, mine.at[1, :, right], last_b, across)
    summed(3)
    far_a.start()
    far_b.start()
    summed(1)
    near_a.start()
    summed(2)
    near_b.start()
    summed(0)
    far_a.wait_recv()
    add(mine.at[2, :, left], first_a.at[1])
    next_a.start()
    far_b.wait_recv()
    add(mine.at[1, :, right], first_b.at[1])
    next_b.start()
    near_a.wait_recv()
    add(mine.at[0, :, left], first_a.at[0])
    near_b.wait_recv()
    add(mine.at[0, :, right], first_b.at[0])

    def finish(where, extra):
        @pl.loop(0, rows // 32)
        def _(r):
            at = pl.ds(pl.multiple_of(r * 32, 32), 32)
            out_ref[at, where] = mine[0, at, where] + extra[at, :]

    next_a.wait_recv()
    finish(left, last_a)
    next_b.wait_recv()
    finish(right, last_b)
    for copy in (*pair.values(), far_a, far_b, near_a, near_b, next_a, next_b):
        copy.wait_send()


def reduce_blocks(part, collective_id):
    seq_len, cols = part.shape
    rows = seq_len // 8
    return pl.pallas_call(
        reduce_kernel,
        out_shape=jax.ShapeDtypeStruct((rows, cols), part.dtype),
        in_specs=[pl.BlockSpec(memory_space=pl.ANY)],
        out_specs=pl.BlockSpec(memory_space=pltpu.VMEM),
        scratch_shapes=[
            pltpu.VMEM((4, rows, cols), part.dtype),
            pltpu.VMEM((4, rows, cols), part.dtype),
            pltpu.VMEM((2, rows, cols // 2), part.dtype),
            pltpu.VMEM((2, rows, cols // 2), part.dtype),
            pltpu.VMEM((rows, cols // 2), part.dtype),
            pltpu.VMEM((rows, cols // 2), part.dtype),
            pltpu.SemaphoreType.DMA((10,)),
            pltpu.SemaphoreType.DMA((10,)),
            pltpu.SemaphoreType.DMA((4,)),
        ],
        compiler_params=pltpu.CompilerParams(collective_id=collective_id, has_side_effects=True, vmem_limit_bytes=40 * MIB),
        cost_estimate=cost(60000),
        name='reduce_blocks',
    )(part.reshape(8, rows, cols))


def swap_halves(values, head_dim):
    half = head_dim // 2
    lanes = values.shape[1]
    lane = lax.broadcasted_iota(jnp.int32, values.shape, 1)
    return jnp.where(lane % head_dim < half, pltpu.roll(values, lanes - half, 1), pltpu.roll(values, half, 1))


def rotate_lanes(values, cos_lanes, sin_lanes, head_dim):
    return values * cos_lanes + swap_halves(values, head_dim) * sin_lanes


def qkv_kernel(head_dim, me_ref, x_ref, gain_ref, w_ref, cos_ref, sin_ref, q_ref, k_ref, v_ref, u_rows_ref, x_rows_ref):
    width = q_ref.shape[1]
    hidden = x_ref[:].astype(F32)
    inv_rms = inverse_rms(hidden)
    normed = (hidden * inv_rms * gain_ref[:]).astype(B16)
    own = pl.ds(pl.multiple_of(me_ref[0] * u_rows_ref.shape[1], 128), u_rows_ref.shape[1])
    scaled = x_ref[:, own].astype(F32) * inv_rms
    x_rows_ref[:] = scaled
    u_rows_ref[:] = (scaled * gain_ref[:, own]).astype(B16)
    lin = jnp.dot(normed, w_ref[:], preferred_element_type=F32).astype(B16)
    cos_lanes, sin_lanes = cos_ref[:], sin_ref[:]
    rotated = [rotate_lanes(lin[:, i:i + 128].astype(F32), cos_lanes, sin_lanes, head_dim).astype(B16) for i in range(0, width + 128, 128)]
    q_ref[:] = jnp.concatenate(rotated[:-1], axis=1)
    k_ref[:] = rotated[-1][:, :head_dim]
    v_ref[:] = lin[:, width + head_dim:]


def project_qkv(me, x_full, gain, w_qkv, cos_lanes, sin_lanes, head_dim):
    seq_len, model_dim = x_full.shape
    width = w_qkv.shape[1] - 2 * head_dim
    part = BLOCK

    def tile(cols):
        return pl.BlockSpec((BLOCK, cols), lambda i, me_ref: (i, 0))

    return pl.pallas_call(
        functools.partial(qkv_kernel, head_dim),
        grid_spec=pltpu.PrefetchScalarGridSpec(
            num_scalar_prefetch=1,
            grid=(seq_len // BLOCK,),
            in_specs=[tile(model_dim), whole_block((1, model_dim)), whole_block(w_qkv.shape), tile(128), tile(128)],
            out_specs=(tile(width), tile(head_dim), tile(head_dim), tile(part), tile(part)),
        ),
        out_shape=(
            jax.ShapeDtypeStruct((seq_len, width), B16),
            jax.ShapeDtypeStruct((seq_len, head_dim), B16),
            jax.ShapeDtypeStruct((seq_len, head_dim), B16),
            jax.ShapeDtypeStruct((seq_len, part), B16),
            jax.ShapeDtypeStruct((seq_len, part), F32),
        ),
        compiler_params=pltpu.CompilerParams(vmem_limit_bytes=32 * MIB),
        cost_estimate=cost(3000),
        name='project_qkv',
    )(me.reshape(1), x_full, gain, w_qkv, cos_lanes, sin_lanes)


def hold_weights(me_ref, held_refs, block_refs):
    count = held_refs[0].shape[0]

    @pl.when(pl.program_id(0) == 0)
    def _():
        for i, held in enumerate(held_refs):
            for k, ref in zip((0,) + XOR_ORDER, block_refs[i * count:(i + 1) * count]):
                held[lax.bitwise_xor(me_ref[0], k)] = ref[0]

    return [held[:].reshape(count * held.shape[1], held.shape[2]) for held in held_refs]


def mlp_forward_kernel(me_ref, h_ref, gain_ref, down_ref, *refs):
    weight_refs, out_refs, held_refs = refs[:-7], refs[-7:-2], refs[-2:]
    m_ref, gate_ref, up_ref, glu_ref, y_ref = out_refs
    w_gate, w_up = hold_weights(me_ref, held_refs, weight_refs)
    hidden = h_ref[:].astype(F32)
    mlp_in = (hidden * inverse_rms(hidden) * gain_ref[:]).astype(B16)
    m_ref[:] = mlp_in
    gate_ref[:] = gate = jnp.dot(mlp_in, w_gate, preferred_element_type=F32).astype(B16)
    up_ref[:] = up = jnp.dot(mlp_in, w_up, preferred_element_type=F32).astype(B16)
    glu_ref[:] = glu = gated_unit(gate.astype(F32), up.astype(F32)).astype(B16)
    y_ref[:] = jnp.dot(glu, down_ref[:], preferred_element_type=F32)


def mlp_backward_kernel(me_ref, gate_ref, up_ref, dy_ref, down_ref, *refs):
    weight_refs, (da_ref, db_ref, dm_ref), held_refs = refs[:-5], refs[-5:-2], refs[-2:]
    w_gate, w_up = hold_weights(me_ref, held_refs, weight_refs)
    gate, up = gate_ref[:].astype(F32), up_ref[:].astype(F32)
    d_glu = dot_f32(dy_ref[:], down_ref[:], ((1,), (1,))).astype(B16).astype(F32)
    sig = jax.nn.sigmoid(gate)
    silu = gate * sig
    da_ref[:] = d_gate = (d_glu * up * (sig + silu * (1.0 - sig))).astype(B16)
    db_ref[:] = d_up = (d_glu * silu).astype(B16)
    dm_ref[:] = dot_f32(d_gate, w_gate, ((1,), (1,))) + dot_f32(d_up, w_up, ((1,), (1,)))


def token_tile(cols):
    return pl.BlockSpec((MLP_BLOCK, cols), lambda i, me_ref: (i, 0))


def whole_block(shape):
    return pl.BlockSpec(shape, lambda *ids: (0,) * len(shape))


def mlp_call(kernel, me, operands, operand_specs, weights, out_cols, out_types, flops):
    seq_len = operands[0].shape[0]
    count, rows, part = weights[0].shape
    own_spec = pl.BlockSpec((1, rows, part), lambda i, me_ref: (me_ref[0], 0, 0))
    came_spec = whole_block((1, rows, part))
    weight_specs = ([own_spec] + [came_spec] * (count - 1)) * 2
    return pl.pallas_call(
        kernel,
        grid_spec=pltpu.PrefetchScalarGridSpec(
            num_scalar_prefetch=1,
            grid=(seq_len // MLP_BLOCK,),
            in_specs=operand_specs + weight_specs,
            out_specs=tuple(token_tile(cols) for cols in out_cols),
            scratch_shapes=[pltpu.VMEM((count, rows, part), B16), pltpu.VMEM((count, rows, part), B16)],
        ),
        out_shape=tuple(jax.ShapeDtypeStruct((seq_len, cols), dtype) for cols, dtype in zip(out_cols, out_types)),
        compiler_params=pltpu.CompilerParams(vmem_limit_bytes=60 * MIB),
        cost_estimate=cost(flops),
    )(me.reshape(1), *operands, *weights)


def ffn_grad_kernel(me_ref, m_ref, da_ref, db_ref, *refs):
    out_refs, (da_t, db_t) = refs[:-2], refs[-2:]
    count = len(out_refs) // 2
    step = pl.program_id(0)

    @pl.when(step == 0)
    def _():
        da_t[:] = da_ref[:].T
        db_t[:] = db_ref[:].T

    gate_grad = jnp.dot(da_t[:], m_ref[:], preferred_element_type=F32)
    up_grad = jnp.dot(db_t[:], m_ref[:], preferred_element_type=F32)
    for k in range(count):
        @pl.when(step == k)
        def _():
            out_refs[k][0] = gate_grad
            out_refs[count + k][0] = up_grad


def ffn_grads(me, mlp_in, d_gate_act, d_up_act, count):
    seq_len, model_dim = mlp_in.shape
    rows, part = model_dim // count, d_gate_act.shape[1]
    shape = jax.ShapeDtypeStruct((1, part, rows), F32)
    blocks = pl.pallas_call(
        ffn_grad_kernel,
        grid_spec=pltpu.PrefetchScalarGridSpec(
            num_scalar_prefetch=1,
            grid=(count,),
            in_specs=[pl.BlockSpec((seq_len, rows), lambda k, me_ref: (0, lax.bitwise_xor(me_ref[0], k)))] + [whole_block((seq_len, part))] * 2,
            out_specs=(whole_block(shape.shape),) * (2 * count),
            scratch_shapes=[pltpu.VMEM((part, seq_len), B16), pltpu.VMEM((part, seq_len), B16)],
        ),
        out_shape=(shape,) * (2 * count),
        compiler_params=pltpu.CompilerParams(vmem_limit_bytes=56 * MIB),
        cost_estimate=cost(12000),
        name='ffn_grads',
    )(me.reshape(1), mlp_in, d_gate_act, d_up_act)
    return blocks[:count], blocks[count:]


def join_kernel(me_ref, *refs):
    blocks, out_ref, held = refs[:-2], refs[-2], refs[-1]
    for k, ref in zip((0,) + XOR_ORDER, blocks):
        held[lax.bitwise_xor(me_ref[0], k)] = ref[0]
    count, width, rows = held.shape
    for pair in range(count // 2):
        out_ref[:, pair * 2 * width:(pair + 1) * 2 * width] = held[2 * pair:2 * pair + 2].reshape(2 * width, rows).T


def join_columns(me, own, came):
    count = 1 + len(came)
    width, rows = own.shape[1:]
    tile = 128
    spec = pl.BlockSpec((1, width, tile), lambda i, me_ref: (0, 0, i))
    return pl.pallas_call(
        join_kernel,
        grid_spec=pltpu.PrefetchScalarGridSpec(
            num_scalar_prefetch=1,
            grid=(rows // tile,),
            in_specs=[spec] * count,
            out_specs=pl.BlockSpec((tile, count * width), lambda i, me_ref: (i, 0)),
            scratch_shapes=[pltpu.VMEM((count, width, tile), own.dtype)],
        ),
        out_shape=jax.ShapeDtypeStruct((rows, count * width), own.dtype),
        compiler_params=pltpu.CompilerParams(vmem_limit_bytes=32 * MIB),
        cost_estimate=cost(1),
        name='join_columns',
    )(me.reshape(1), own, *came)


def pair_heads_kernel(k_ref, v_ref, out_ref):
    width = k_ref.shape[1] // 4
    parts = [ref[:, h * width:(h + 1) * width] for h in range(4) for ref in (k_ref, v_ref)]
    out_ref[:] = jnp.concatenate(parts, axis=1)


def pair_heads(wk_rows, wv_rows):
    rows, cols = wk_rows.shape
    return pl.pallas_call(pair_heads_kernel, out_shape=jax.ShapeDtypeStruct((rows, 2 * cols), B16), name='pair_heads')(wk_rows, wv_rows)


def normed_grad_kernel(width, head_dim, g_ref, x_ref, wq_ref, wkv_ref, cos_ref, sin_ref, dkv_ref, du_ref, dg_ref, acc_ref, share_ref):
    step = pl.program_id(0)
    half = head_dim // 2

    @pl.when(step == 0)
    def _():
        acc_ref[:] = jnp.zeros_like(acc_ref)

    acc_ref[:] += jnp.dot(wq_ref[:], g_ref[0, :width, :], preferred_element_type=F32)
    share = g_ref[0, width:width + 2 * head_dim, :].astype(F32)

    @pl.when(step % 2 == 0)
    def _():
        share_ref[:] = share

    @pl.when(step % 2 == 1)
    def _():
        summed = (share_ref[:] + share).astype(B16)
        first, second = summed[:half].astype(F32), summed[half:head_dim].astype(F32)
        cos_rows, sin_rows = cos_ref[:], sin_ref[:]
        dk = jnp.concatenate([first * cos_rows + second * sin_rows, second * cos_rows - first * sin_rows], axis=0).astype(B16)
        dkv = jnp.concatenate([dk, summed[head_dim:]], axis=0)
        dkv_ref[0] = dkv
        acc_ref[:] += jnp.dot(wkv_ref[:], dkv, preferred_element_type=F32)

    @pl.when(step == pl.num_programs(0) - 1)
    def _():
        d_normed = acc_ref[:].T.astype(B16)
        du_ref[:] = d_normed
        dg_ref[:] = jnp.sum(d_normed.astype(F32) * x_ref[:], axis=0, keepdims=True)


def normed_grads(gathered, x_rows, wq_rows, wkv_rows, cos_t, sin_t, head_dim):
    count, height, seq_len = gathered.shape
    rows = x_rows.shape[1]
    width = wq_rows.shape[1] // count

    return pl.pallas_call(
        functools.partial(normed_grad_kernel, width, head_dim),
        grid=(count,),
        in_specs=[
            pl.BlockSpec((1, height, seq_len), lambda e: (e, 0, 0)),
            whole_block(x_rows.shape),
            pl.BlockSpec((rows, width), lambda e: (0, e)),
            pl.BlockSpec((rows, 2 * head_dim), lambda e: (0, e // 2)),
            whole_block(cos_t.shape),
            whole_block(sin_t.shape),
        ],
        out_specs=(pl.BlockSpec((1, 2 * head_dim, seq_len), lambda e: (e // 2, 0, 0)), whole_block((seq_len, rows)), whole_block((1, rows))),
        out_shape=(
            jax.ShapeDtypeStruct((count // 2, 2 * head_dim, seq_len), B16),
            jax.ShapeDtypeStruct((seq_len, rows), B16),
            jax.ShapeDtypeStruct((1, rows), F32),
        ),
        scratch_shapes=[pltpu.VMEM((rows, seq_len), F32), pltpu.VMEM((2 * head_dim, seq_len), F32)],
        compiler_params=pltpu.CompilerParams(vmem_limit_bytes=40 * MIB),
        cost_estimate=cost(3000),
        name='normed_grads',
    )(gathered, x_rows, wq_rows, wkv_rows, cos_t, sin_t)


def qkv_grad_kernel(width, head_dim, g_ref, dkv_ref, u_ref, dwq_ref, dwk_ref, dwv_ref):
    step = pl.program_id(0)
    dwq_ref[:] = jnp.dot(g_ref[0, :width, :], u_ref[:], preferred_element_type=F32).T
    kv_heads = dkv_ref.shape[0]

    @pl.when(step == 0)
    def _():
        both = jnp.dot(dkv_ref[:].reshape(kv_heads * 2 * head_dim, -1), u_ref[:], preferred_element_type=F32).T
        for out_ref, offset in ((dwk_ref, 0), (dwv_ref, head_dim)):
            out_ref[:] = jnp.concatenate([both[:, h * 2 * head_dim + offset:h * 2 * head_dim + offset + head_dim] for h in range(kv_heads)], axis=1)


def qkv_grads(gathered, dkv_t, u_rows, width, head_dim):
    count, height, seq_len = gathered.shape
    rows = u_rows.shape[1]
    kv_width = dkv_t.shape[0] * head_dim
    kv_spec = whole_block((rows, kv_width))
    return pl.pallas_call(
        functools.partial(qkv_grad_kernel, width, head_dim),
        grid=(count,),
        in_specs=[
            pl.BlockSpec((1, height, seq_len), lambda e: (e, 0, 0)),
            whole_block(dkv_t.shape),
            whole_block(u_rows.shape),
        ],
        out_specs=(pl.BlockSpec((rows, width), lambda e: (0, e)), kv_spec, kv_spec),
        out_shape=(
            jax.ShapeDtypeStruct((rows, count * width), F32),
            jax.ShapeDtypeStruct((rows, kv_width), F32),
            jax.ShapeDtypeStruct((rows, kv_width), F32),
        ),
        compiler_params=pltpu.CompilerParams(vmem_limit_bytes=40 * MIB),
        cost_estimate=cost(3000),
        name='qkv_grads',
    )(gathered, dkv_t, u_rows)


def solution(mesh):
    n_dev = mesh.shape['sp']
    gather_rows = functools.partial(lax.all_gather, axis_name='sp', axis=0, tiled=True)
    scatter_rows = functools.partial(lax.psum_scatter, axis_name='sp', scatter_dimension=0, tiled=True)
    swap_blocks = functools.partial(lax.all_to_all, axis_name='sp', split_axis=0, concat_axis=0, tiled=True)

    def send_blocks(others, order=XOR_ORDER):
        others = lax.optimization_barrier(tuple(with_layout_constraint(other, Layout((0, 1, 2))) for other in others))
        came = []
        for k, other in zip(order, others):
            came.append(with_layout_constraint(lax.ppermute(other, 'sp', [(i, i ^ k) for i in range(n_dev)]), Layout((0, 1, 2))))
        return came

    def pick_blocks(blocks):
        me = lax.axis_index('sp')
        return [lax.dynamic_index_in_dim(blocks, lax.bitwise_xor(me, k), axis=0, keepdims=True) for k in XOR_ORDER]

    def after(value, *others):
        return lax.optimization_barrier((value,) + others)[0]

    def to_tokens(columns):
        blocks = swap_blocks(columns.reshape(n_dev, -1, columns.shape[1]))
        return blocks.transpose(1, 0, 2).reshape(blocks.shape[1], -1)

    def layer_step(x_in, positions, d_out, norm1_gain, norm2_gain, w_q, w_k, w_v, w_o, w_gate, w_up, w_down):
        tokens, model_dim = x_in.shape
        rows = model_dim // n_dev
        seq_len = tokens * n_dev
        q_heads, head_dim = w_q.shape[1:]
        kv_heads = w_k.shape[1]
        heads = q_heads // n_dev
        width = heads * head_dim
        kv_repeat = n_dev // kv_heads
        ffn_part = w_down.shape[0]
        me = lax.axis_index('sp')
        own_rows = functools.partial(lax.dynamic_slice_in_dim, start_index=me * rows, slice_size=rows, axis=1)

        x_full = gather_rows(x_in)
        wq_rows = w_q.reshape(rows, q_heads * head_dim)
        wk_rows = w_k.reshape(rows, kv_heads * head_dim)
        wv_rows = w_v.reshape(rows, kv_heads * head_dim)
        wo_rows = w_o.reshape(width, model_dim)

        wq_blocks = wq_rows.reshape(rows, n_dev, width).transpose(1, 0, 2)
        wk_blocks = jnp.repeat(w_k.transpose(1, 0, 2), kv_repeat, axis=0)
        wv_blocks = jnp.repeat(w_v.transpose(1, 0, 2), kv_repeat, axis=0)
        qkv_blocks = jnp.concatenate([wq_blocks, wk_blocks, wv_blocks], axis=2)
        lane_width = qkv_blocks.shape[2]
        small = jnp.stack([norm1_gain, norm2_gain, (positions // 128).astype(B16), (positions % 128).astype(B16)])
        small = jnp.pad(small, ((0, 12), (0, lane_width - rows)))
        small = jnp.broadcast_to(small[None], (n_dev,) + small.shape)
        qkv_cols = swap_blocks(jnp.concatenate([qkv_blocks, small], axis=1))
        w_qkv = qkv_cols[:, :rows].reshape(model_dim, lane_width)
        gain1 = qkv_cols[:, rows, :rows].reshape(model_dim).astype(F32)
        gain2 = qkv_cols[:, rows + 1, :rows].reshape(model_dim).astype(F32)
        pos_all = (qkv_cols[:, rows + 2, :rows].astype(F32) * 128.0 + qkv_cols[:, rows + 3, :rows].astype(F32)).reshape(seq_len)

        wo_full = gather_rows(wo_rows)
        dy_full = gather_rows(d_out)
        gate_blocks = w_gate.reshape(rows, n_dev, ffn_part).transpose(1, 0, 2)
        up_blocks = w_up.reshape(rows, n_dev, ffn_part).transpose(1, 0, 2)
        gate_others, up_others = pick_blocks(gate_blocks), pick_blocks(up_blocks)
        gate_came = send_blocks(gate_others[:FIRST], XOR_ORDER[:FIRST])
        gate_others, up_others, x_full = lax.optimization_barrier((gate_others[FIRST:], up_others, x_full))
        gate_came, up_came = gate_came + send_blocks(gate_others, XOR_ORDER[FIRST:]), send_blocks(up_others)

        cos_tab, sin_tab = rope_tables(pos_all, head_dim)
        cos_tab, sin_tab = cos_tab[:, 0], sin_tab[:, 0]
        cos_lanes = jnp.tile(cos_tab, (1, 4))
        sin_lanes = jnp.tile(jnp.concatenate([-sin_tab, sin_tab], axis=1), (1, 2))
        q_rot, k_rot, v_lin, u_rows, x_rows = project_qkv(me, x_full, gain1[None], w_qkv, cos_lanes, sin_lanes, head_dim)
        attn_cols, row_max, inv_sum = attention_forward(q_rot, k_rot, v_lin, heads)
        attn_tok = to_tokens(attn_cols)
        hidden = (x_in.astype(F32) + jnp.dot(attn_tok, wo_full, preferred_element_type=F32)).astype(B16)
        h_full = gather_blocks(hidden, 1)
        wk_late, wv_late = lax.optimization_barrier((wk_rows, wv_rows, hidden))[:2]
        wkv_rows = pair_heads(wk_late, wv_late)
        weights = (gate_blocks, *gate_came, up_blocks, *up_came)
        mlp_in, gate_act, up_act, glu_out, y_part = mlp_call(
            mlp_forward_kernel, me, (h_full, gain2[None], w_down),
            [token_tile(model_dim), whole_block((1, model_dim)), whole_block(w_down.shape)],
            weights, (model_dim, ffn_part, ffn_part, ffn_part, model_dim), (B16, B16, B16, B16, F32), 18_000)
        y_sum = scatter_rows(y_part)
        d_gate_act, d_up_act, d_mlp_part = mlp_call(
            mlp_backward_kernel, me, (gate_act, up_act, dy_full, w_down),
            [token_tile(ffn_part), token_tile(ffn_part), token_tile(model_dim), whole_block(w_down.shape)],
            weights, (ffn_part, ffn_part, model_dim), (B16, B16, F32), 18_000)
        d_gate_blocks, d_up_blocks = ffn_grads(me, mlp_in, d_gate_act, d_up_act, n_dev)
        d_gate_others = [d_gate_blocks[k] for k in XOR_ORDER]
        d_up_others = [d_up_blocks[k] for k in XOR_ORDER]
        cos_t, sin_t = cos_tab.T, sin_tab.T
        d_mlp_part, d_up_others, d_gate_others, cos_t, sin_t, wkv_rows = lax.optimization_barrier((d_mlp_part, d_up_others, d_gate_others, cos_t, sin_t, wkv_rows))
        d_gate_came = send_blocks(d_gate_others[:NOW], XOR_ORDER[:NOW])
        d_mlp_sum = reduce_blocks(d_mlp_part, 4)
        d_mlp_in = d_mlp_sum.astype(B16).astype(F32)
        hidden_f = hidden.astype(F32)
        inv2 = inverse_rms(hidden_f)
        d_hidden = (d_out.astype(F32) + norm_backward(d_mlp_in, hidden_f, inv2, gain2)).astype(B16)
        d_g2_part = jnp.sum(d_mlp_in * hidden_f * inv2, axis=0)
        dh_full = gather_blocks(d_hidden, 2)
        d_gate_came += send_blocks(after(d_gate_others[NOW:], dh_full), XOR_ORDER[NOW:])
        d_up_came = send_blocks(after(d_up_others[:EARLY], dh_full), XOR_ORDER[:EARLY])

        d_attn = jnp.einsum('td,cd->tc', dh_full, wo_rows, preferred_element_type=F32).astype(B16)
        dq_t, dk_t, dv_t = attention_backward(q_rot, d_attn, k_rot, v_lin, row_max, inv_sum, cos_lanes, sin_lanes, heads)
        piece_hi = lax.reduce_precision(d_g2_part, 8, 7)
        piece_mid = lax.reduce_precision(d_g2_part - piece_hi, 8, 7)
        piece_lo = lax.reduce_precision(d_g2_part - piece_hi - piece_mid, 8, 7)
        pieces = jnp.pad(jnp.stack([piece_hi, piece_mid, piece_lo]).astype(B16), ((0, 13), (0, 0)))
        dqkv_t = gather_rows(jnp.concatenate([dq_t, dk_t, dv_t, pieces], axis=0)).reshape(n_dev, width + 2 * head_dim + 16, seq_len)
        d_g2 = jnp.sum(own_rows(dqkv_t[:, width + 2 * head_dim:width + 2 * head_dim + 3].reshape(-1, seq_len)).astype(F32), axis=0)
        glu_late, o_late = lax.optimization_barrier((glu_out, attn_cols, dk_t))[:2]
        d_down = jnp.einsum('tf,td->fd', glu_late, dy_full, preferred_element_type=F32)
        d_wo = jnp.einsum('tc,td->cd', o_late, dh_full, preferred_element_type=F32)
        d_gate = join_columns(me, d_gate_blocks[0], d_gate_came)
        dqkv_t, d_down, d_wo, d_gate = lax.optimization_barrier((dqkv_t, d_down, d_wo, d_gate))
        d_up_came += send_blocks(after(d_up_others[EARLY:], dqkv_t), XOR_ORDER[EARLY:])
        d_up = join_columns(me, d_up_blocks[0], d_up_came)
        y_out = (hidden_f + y_sum).astype(B16)

        dkv_t, d_norm_cols, d_g1 = normed_grads(dqkv_t, x_rows, wq_rows, wkv_rows, cos_t, sin_t, head_dim)
        d_wq, d_wk, d_wv = qkv_grads(dqkv_t, dkv_t, u_rows, width, head_dim)
        d_g1 = d_g1[0]
        d_normed = to_tokens(d_norm_cols).astype(F32)
        x_f32 = x_in.astype(F32)
        d_x = (d_hidden.astype(F32) + norm_backward(d_normed, x_f32, inverse_rms(x_f32), gain1)).astype(B16)
        return (y_out, d_x, d_g1, d_g2, d_wq.reshape(w_q.shape), d_wk.reshape(w_k.shape), d_wv.reshape(w_v.shape), d_wo.reshape(w_o.shape), d_gate, d_up, d_down)

    all_rows = P('sp')
    return jax.shard_map(layer_step, mesh=mesh, in_specs=(all_rows,) * 12, out_specs=(all_rows,) * 11, check_vma=False)
```
